256 devices in a mesh: dev: 128 (over x, z, y), rep: 2 (over core).
Axes of the slice: x: 4, y: 4, z: 8, core: 2. Of those that a mesh axis runs over, the one named last changes fastest.
Arguments:
- node_features: bfloat16 [8192, 2, 3136], P('dev', 'rep'), may hold values from -6 to 6
- src_node: int32 [128, 128, 2], P('dev'), may hold values from 0 to 63
- dst_node: int32 [128, 128, 2], P('dev'), may hold values from 0 to 63
- counts: int32 [128, 128], P('dev'), may hold values from 1 to 2, as said below
- rotation: bfloat16 [128, 128, 2, 235], P('dev'), may hold values from -2 to 2
- w_zero: bfloat16 [896, 2, 448], P(None, 'rep'), may hold values from -0.1875 to 0.1875
- w_one: bfloat16 [2, 768, 2, 384], P(None, None, 'rep'), may hold values from -0.15625 to 0.15625
- w_two: bfloat16 [2, 640, 2, 320], P(None, None, 'rep'), may hold values from -0.15625 to 0.15625
- norm_gain: float32 [2, 3136], P('rep'), may hold values from 0.5 to 1.5
Outputs:
- updated: bfloat16 [8192, 2, 3136], P('dev', 'rep')
The draws below stay inside these ranges and needn't reach their ends.
Inputs may be any that keep to these rules, and one draw needn't show every extreme that they name: Slots i < counts[s, d] hold edges, the others padding; in every draw some destination device receives 2 edges from every source device.
All inputs are finite; a program needn't handle non-finite values.
Results may differ from the reference program's by a relative error of at most 0.0054.
Values may be sent and summed in bfloat16 or wider, within the bound.
A program may use at most 64 MiB of HBM per device.

```python
import jax
import jax.numpy as jnp
from jax import lax

C = 128
COEFFS = 49
ROT = 235
NODE_DEV = 64
CAP = 2
CH = 64
NODES = 8192
N_DEV = 128
N_REP = 2


def draw_counts(key, part):
    counts_base = jax.random.randint(jax.random.fold_in(key, 11), (N_DEV, N_DEV), 1, CAP + 1)
    hot_dest = jax.random.randint(jax.random.fold_in(key, 12), (2,), 0, N_DEV)
    column = jnp.arange(N_DEV)
    is_hot = (column[None, :] == hot_dest[0]) | (column[None, :] == hot_dest[1])
    return jnp.where(is_hot, CAP, counts_base).astype(jnp.int32)


def touch_ends(values, key, least, largest):
    longest = values.shape.index(max(values.shape))
    spots = []
    for shift in (0, 1):
        where = [jax.random.randint(jax.random.fold_in(key, axis), (), 0, length) for axis, length in enumerate(values.shape)]
        where[longest] = (where[longest] + shift) % values.shape[longest]
        spots.append(tuple(where))
    return values.at[spots[0]].set(least).at[spots[1]].set(largest)


def block_levels(rng, shape, cuts, least, largest):
    def one(dim, blocks):
        heights = jax.random.uniform(jax.random.fold_in(jax.random.fold_in(rng, 6), dim), (blocks,), jnp.float32, least / len(cuts), largest / len(cuts))
        return jnp.repeat(jnp.exp(heights), shape[dim] // blocks).reshape((-1,) + (1,) * (len(shape) - dim - 1))

    gain = one(*cuts[0])
    for cut in cuts[1:]:
        gain = gain * one(*cut)
    return gain


def centred(own_key, shape, spread, most, cuts=(), dtype=jnp.bfloat16):
    values = spread * jax.random.normal(own_key, shape, jnp.float32)
    if cuts:
        values = values * block_levels(own_key, shape, cuts, -0.22, 0.18)
    return jnp.clip(values, -most, most).astype(dtype)


def setup_inputs(seed: int = 0) -> dict:
    key_list = jax.random.split(jax.random.key(seed), 10)
    return {
        "node_features": centred(key_list[0], (NODES, N_REP, COEFFS * CH), 1.0, 6.0, ((0, 128), (1, 2))),
        "src_node": touch_ends(jax.random.randint(key_list[1], (N_DEV, N_DEV, CAP), 0, NODE_DEV), jax.random.fold_in(key_list[1], 1), 0, NODE_DEV - 1).astype(jnp.int32),
        "dst_node": touch_ends(jax.random.randint(key_list[2], (N_DEV, N_DEV, CAP), 0, NODE_DEV), jax.random.fold_in(key_list[2], 1), 0, NODE_DEV - 1).astype(jnp.int32),
        "counts": draw_counts(jax.random.fold_in(key_list[9], 71), 0),
        "rotation": centred(key_list[4], (N_DEV, N_DEV, CAP, ROT), 0.35, 2.0, ((0, 128),)),
        "w_zero": centred(key_list[5], (7 * C, N_REP, 7 * CH), (7 * C) ** -0.5, 0.1875, ((1, 2),)),
        "w_one": centred(key_list[6], (2, 6 * C, N_REP, 6 * CH), (12 * C) ** -0.5, 0.15625, ((2, 2),)),
        "w_two": centred(key_list[7], (2, 5 * C, N_REP, 5 * CH), (10 * C) ** -0.5, 0.15625, ((2, 2),)),
        "norm_gain": jnp.clip(1.0 + 0.1 * jax.random.normal(key_list[8], (N_REP, COEFFS * CH), jnp.float32), 0.5, 1.5),
    }


def frame_slot(degree, order):
    if order == 0:
        return degree
    if order == 1:
        return 6 + degree
    if order == -1:
        return 12 + degree
    if order == 2:
        return 17 + degree
    return 22 + degree

def frame_tables():
    offsets = []
    places = []
    spot = 0
    for degree in range(7):
        reach = min(degree, 2)
        offsets.append(spot)
        spot += (2 * degree + 1) * (2 * reach + 1)
        places.append([frame_slot(degree, order) for order in range(-reach, reach + 1)])
    return (offsets, places)

def rounded(value):
    return lax.optimization_barrier(value.astype(jnp.bfloat16)).astype(jnp.float32)

def block_of(rotation, offsets, degree):
    reach = min(degree, 2)
    span = 2 * degree + 1
    height = 2 * reach + 1
    piece = rotation[:, offsets[degree]:offsets[degree] + height * span]
    return piece.reshape(rotation.shape[0], height, span).astype(jnp.float32)

def frame(coeffs, rotation):
    offsets, places = frame_tables()
    pieces = []
    for degree in range(7):
        matrix = block_of(rotation, offsets, degree)
        part = coeffs[:, degree * degree:degree * degree + 2 * degree + 1, :].astype(jnp.float32)
        pieces.append(lax.optimization_barrier(jnp.sum(matrix[:, :, :, None] * part[:, None, :, :], axis=2)))
    listing = sorted(((places[degree][row], degree, row) for degree in range(7) for row in range(len(places[degree]))))
    return jnp.concatenate([pieces[degree][:, row:row + 1, :] for place, degree, row in listing], axis=1)

def unframe(framed, rotation):
    offsets, places = frame_tables()
    parts = []
    for degree in range(7):
        matrix = block_of(rotation, offsets, degree)
        chosen = jnp.concatenate([framed[:, place:place + 1, :] for place in places[degree]], axis=1).astype(jnp.float32)
        parts.append(lax.optimization_barrier(jnp.sum(matrix[:, :, :, None] * chosen[:, :, None, :], axis=1)))
    return jnp.concatenate(parts, axis=1)

def mix_orders(rotated, zero_mat, one_mats, two_mats):
    batch = rotated.shape[0]
    out_width = zero_mat.shape[1] // 7
    flat_zero = rotated[:, 0:7, :].reshape(batch, -1)
    result = [jnp.dot(flat_zero, zero_mat, preferred_element_type=jnp.float32).reshape(batch, 7, out_width)]
    for first, count, mats in ((7, 6, one_mats), (19, 5, two_mats)):
        plus = rotated[:, first:first + count, :].reshape(batch, -1)
        minus = rotated[:, first + count:first + 2 * count, :].reshape(batch, -1)
        upper = jnp.dot(plus, mats[0], preferred_element_type=jnp.float32) - jnp.dot(minus, mats[1], preferred_element_type=jnp.float32)
        lower = jnp.dot(plus, mats[1], preferred_element_type=jnp.float32) + jnp.dot(minus, mats[0], preferred_element_type=jnp.float32)
        result.append(upper.reshape(batch, count, out_width))
        result.append(lower.reshape(batch, count, out_width))
    return jnp.concatenate(result, axis=1)

def reference(node_features, src_node, dst_node, counts, rotation, w_zero, w_one, w_two, norm_gain):
    nodes, halves, flat = node_features.shape
    half_width = flat // 49
    width = halves * half_width
    full = node_features.reshape(nodes, halves, 49, half_width).transpose(0, 2, 1, 3).reshape(nodes, 49, width)
    zero_mat = w_zero.reshape(7 * width, halves, 7, half_width).transpose(0, 2, 1, 3).reshape(7 * width, 7 * width)
    one_mats = w_one.reshape(2, 6 * width, halves, 6, half_width).transpose(0, 1, 3, 2, 4).reshape(2, 6 * width, 6 * width)
    two_mats = w_two.reshape(2, 5 * width, halves, 5, half_width).transpose(0, 1, 3, 2, 4).reshape(2, 5 * width, 5 * width)
    slots = jnp.arange(CAP).astype(jnp.int32)
    owners = jnp.arange(N_DEV).astype(jnp.int32)

    def one_source(total, source):
        sources = (source * NODE_DEV + src_node[source].reshape(-1)).astype(jnp.int32)
        gathered = jnp.take(full, sources, axis=0)
        rot_rows = rotation[source].reshape(-1, 235)
        rotated = rounded(frame(gathered, rot_rows)).astype(jnp.bfloat16)
        edge_out = rounded(mix_orders(rotated, zero_mat, one_mats, two_mats))
        back = rounded(unframe(edge_out, rot_rows))
        live = (slots[None, :] < counts[source][:, None]).reshape(-1).astype(jnp.float32)
        back = back * live[:, None, None]
        targets = (owners[:, None] * NODE_DEV + dst_node[:, source, :]).reshape(-1).astype(jnp.int32)
        return (total.at[targets].add(back), None)
    total, unused = lax.scan(one_source, jnp.zeros((nodes, 49, width), jnp.float32), owners)
    mean_sq = lax.optimization_barrier(jnp.sum(total * total, axis=(1, 2))) / (49 * width)
    normed = total * lax.rsqrt(mean_sq + 1e-06)[:, None, None]
    normed = normed.reshape(nodes, 49, halves, half_width).transpose(0, 2, 1, 3).reshape(nodes, halves, flat)
    updated = node_features.astype(jnp.float32) + norm_gain[None].astype(jnp.float32) * normed
    return updated.astype(jnp.bfloat16)
```

```python
import functools

import jax
import jax.numpy as jnp
from jax import lax
from jax.experimental import pallas as pl
from jax.experimental.pallas import tpu as pltpu
from jax.sharding import PartitionSpec as P

MESH = pl.DeviceIdType.MESH
F32 = jnp.float32
BF16 = jnp.bfloat16

SLOTS = 128
ROWS = 256
CHUNKS = 4
CROWS = ROWS // CHUNKS
CSLOTS = SLOTS // CHUNKS
SELF = 7
TILES = 15
DEGREES = range(7)


def reach(l):
    return min(l, 2)


def frame_slot(degree, order):
    if order == 0:
        return degree
    if order == 1:
        return 6 + degree
    if order == -1:
        return 12 + degree
    if order == 2:
        return 17 + degree
    return 22 + degree


def arranged(l, a):
    start = sum((2 * m + 1) * (2 * reach(m) + 1) for m in range(l))
    spot = start + (a + reach(l)) * (2 * l + 1)
    return (0, spot) if l <= 4 else (1, spot - 115)


def message_places():
    place = {}
    for r in range(6):
        place[r] = (r // 2, r % 2)
    for r in range(7, 19):
        place[r] = (3 + (r - 7) // 2, (r - 7) % 2)
    for r in range(19, 23):
        place[r] = (9 + (r - 19) // 2, (r - 19) % 2)
    for r in range(24, 28):
        place[r] = (11 + (r - 24) // 2, (r - 24) % 2)
    place[23] = (13, 0)
    place[28] = (13, 1)
    place[6] = (14, 0)
    return place


PLACE = message_places()


def tiles_of(l):
    return range((l * l) // 2, ((l + 1) * (l + 1) - 1) // 2 + 1)


def pattern(lane, l, a, t):
    _, spot = arranged(l, a)
    picks = []
    for k in (2 * t, 2 * t + 1):
        b = k - l * l
        picks.append(spot + b if 0 <= b <= 2 * l else 127)
    return jnp.where(lane < 64, picks[0], picks[1])


def pick(table, index):
    return jnp.take_along_axis(table, index, axis=1, mode="promise_in_bounds")


def nt(a, b):
    return lax.dot_general(a, b, (((1,), (1,)), ((), ())), preferred_element_type=F32)


def nn(a, b):
    return jnp.dot(a, b, preferred_element_type=F32)


def z_step(k):
    return [4, 3, 5, 2, 6, 1, 7, 0][k]


def kernel(
    x_hbm, rt_hbm, src_hbm, dst_hbm, cnt_hbm, wz_hbm, w1_hbm, w2_hbm,
    agg_ref, sq_ref,
    xv, rtv, srcv, dstv, cntv, wz, w1, w2,
    rts, dtab, xs, own, packed, peer, full, msend, mrecv, dsend, drecv, back, sqs, sqr,
    load_sem, ps_sem, pr_sem, ms_sem, mr_sem, ds_sem, dr_sem, q_sem,
):
    me = lax.axis_index("dev")
    rep = lax.axis_index("rep")
    px, pz, py = me // 32, (me // 4) % 8, me % 4
    barrier = pltpu.get_barrier_semaphore()

    def greet(i, carry):
        pl.semaphore_signal(
            barrier, inc=1, device_id={"dev": (me + i + 1) % SLOTS}, device_id_type=MESH
        )
        return carry

    lax.fori_loop(0, SLOTS - 1, greet, 0)
    pl.semaphore_signal(barrier, inc=1, device_id={"rep": 1 - rep}, device_id_type=MESH)

    loads = [
        pltpu.make_async_copy(s, d, load_sem.at[i])
        for i, (s, d) in enumerate(
            [
                (rt_hbm, rtv), (src_hbm, srcv), (dst_hbm, dstv), (cnt_hbm, cntv), (x_hbm, xv),
                (wz_hbm, wz), (w1_hbm, w1), (w2_hbm, w2),
            ]
        )
    ]
    for copy in loads:
        copy.start()
    for copy in loads[:5]:
        copy.wait()

    def spot_of(sign):
        q = lax.broadcasted_iota(jnp.int32, (ROWS, ROWS), 0)
        col = lax.broadcasted_iota(jnp.int32, (ROWS, ROWS), 1)
        slot, i = q // 2, q % 2
        k, r = slot % 8, slot // 8
        h = (k + 1) // 2
        oz = jnp.where(k % 2 == 1, 4 - h, 4 + h)
        ox = r // 4
        oy = (r + r // 4) % 4
        tx = (px + sign * ox + 4) % 4
        tz = (pz + sign * oz + 8) % 8
        ty = (py + sign * oy + 4) % 4
        target = i * SLOTS + (tx * 8 + tz) * 4 + ty
        return jnp.where(col == target, 1.0, 0.0).astype(BF16)

    perm = spot_of(1)
    rts[...] = jnp.zeros_like(rts)
    for i in range(2):
        rts[0:235, i * 128 : (i + 1) * 128] = rtv[:, i, :].astype(F32)
    rows = lax.broadcasted_iota(jnp.int32, (256, 256), 0)
    cols = lax.broadcasted_iota(jnp.int32, (256, 256), 1)
    wanted = jnp.where(rows < 115, rows, jnp.where(rows < 128, 255, jnp.where(rows < 248, rows - 13, 255)))
    sel = jnp.where(wanted == cols, 1.0, 0.0).astype(BF16)
    rcat = nn(sel, rts[...].astype(BF16)).astype(BF16)
    table = nt(perm, rcat)
    dtab[...] = table
    dsend[...] = table.astype(BF16).reshape(SLOTS, 2, 256)

    node = lax.broadcasted_iota(jnp.int32, (64, 128), 0)
    hot = jnp.concatenate(
        [
            jnp.where((srcv[i : i + 1, :] == node) & (cntv[0:1, :] > i), 1.0, 0.0).astype(BF16)
            for i in range(2)
        ],
        axis=1,
    )
    hot_q = nt(perm, hot).astype(BF16)
    for s in range(7):
        xs[:, s * 448 : (s + 1) * 448] = nn(hot_q, xv[:, s * 448 : (s + 1) * 448])
    xs[:, 3136:3200] = jnp.zeros((ROWS, 64), F32)

    lane = lax.broadcasted_iota(jnp.int32, (CROWS, 128), 1)
    low = lane < 64

    def turn(c, carry):
        at = pl.ds(pl.multiple_of(c * CROWS, CROWS), CROWS)
        halves = {}
        for l in DEGREES:
            for a in range(-reach(l), reach(l) + 1):
                piece, _ = arranged(l, a)
                tab = dtab[at, piece * 128 : (piece + 1) * 128]
                acc = None
                for t in tiles_of(l):
                    term = pick(tab, pattern(lane, l, a, t)) * xs[at, t * 128 : (t + 1) * 128]
                    acc = term if acc is None else acc + term
                acc = acc + pltpu.roll(acc, 64, 1)
                row = frame_slot(l, a)
                own[at, row * 128 : (row + 1) * 128] = acc.astype(BF16)
        for t in range(TILES):
            first = own[at, 2 * t * 128 : (2 * t + 1) * 128].astype(F32)
            if t < 14:
                second = own[at, (2 * t + 1) * 128 : (2 * t + 2) * 128].astype(F32)
                first = jnp.where(low, first, second)
            packed[at, t * 128 : (t + 1) * 128] = first.astype(BF16)
        return carry

    lax.fori_loop(0, CHUNKS, turn, 0)

    pl.semaphore_wait(barrier, SLOTS)

    def to_peer(c):
        at = pl.ds(pl.multiple_of(c * CROWS, CROWS), CROWS)
        return pltpu.make_async_remote_copy(
            src_ref=packed.at[at],
            dst_ref=peer.at[at],
            send_sem=ps_sem.at[c],
            recv_sem=pr_sem.at[c],
            device_id={"rep": 1 - rep},
            device_id_type=MESH,
        )

    for c in range(CHUNKS):
        to_peer(c).start()

    tz = [(pz + z_step(k)) % 8 for k in range(8)]

    def send_chunk(c, source, target, send_sem, recv_sem):
        def group(g, carry):
            r = c * (CSLOTS // 8) + g
            tx = (px + r // 4) % 4
            ty = (py + r + r // 4) % 4
            for k in range(8):
                slot = r * 8 + k
                copy = pltpu.make_async_remote_copy(
                    src_ref=source.at[slot],
                    dst_ref=target.at[slot],
                    send_sem=send_sem.at[c],
                    recv_sem=recv_sem.at[c],
                    device_id={"dev": (tx * 8 + tz[k]) * 4 + ty},
                    device_id_type=MESH,
                )
                if k == SELF:

                    @pl.when(r > 0)
                    def _():
                        copy.start()
                else:
                    copy.start()
            return carry

        lax.fori_loop(0, CSLOTS // 8, group, 0)

    def wait_chunk(c, buffer, sem):
        @pl.when(c == 0)
        def _():
            part = buffer.at[pl.ds(0, CSLOTS - 1)]
            pltpu.make_async_copy(part, part, sem.at[0]).wait()

        @pl.when(c > 0)
        def _():
            part = buffer.at[pl.ds(c * CSLOTS, CSLOTS)]
            pltpu.make_async_copy(part, part, sem.at[c]).wait()

    lax.fori_loop(0, CHUNKS, lambda c, n: (send_chunk(c, dsend, drecv, ds_sem, dr_sem), n)[1], 0)
    drecv[SELF] = dsend[SELF]

    for copy in loads[5:]:
        copy.wait()

    mine = (lane // 64) == rep

    def mix(c, carry):
        at = pl.ds(pl.multiple_of(c * CROWS, CROWS), CROWS)
        to_peer(c).wait_recv()
        for t in range(TILES):
            got = peer[at, t * 128 : (t + 1) * 128].astype(F32)
            turned = pltpu.roll(got, 64, 1)
            for half in range(2):
                row = 2 * t + half
                if row < 29:
                    theirs = jnp.where(low, got, turned) if half == 0 else jnp.where(low, turned, got)
                    ours = own[at, row * 128 : (row + 1) * 128].astype(F32)
                    full[:, row * 128 : (row + 1) * 128] = jnp.where(mine, ours, theirs).astype(BF16)
        zero = nt(full[:, 0:896], wz[...])
        p1, m1 = full[:, 896:1664], full[:, 1664:2432]
        p2, m2 = full[:, 2432:3072], full[:, 3072:3712]
        plus1 = nn(p1, w1[0]) - nn(m1, w1[1])
        minus1 = nn(p1, w1[1]) + nn(m1, w1[0])
        plus2 = nt(p2, w2[0]) - nt(m2, w2[1])
        minus2 = nt(p2, w2[1]) + nt(m2, w2[0])
        last = jnp.concatenate([plus2[:, 256:320], minus2[:, 256:320]], axis=1)
        tail = jnp.concatenate([zero[:, 384:448], jnp.zeros((CROWS, 64), F32)], axis=1)
        message = jnp.concatenate(
            [zero[:, 0:384], plus1, minus1, plus2[:, 0:256], minus2[:, 0:256], last, tail], axis=1
        ).astype(BF16)
        spot = pl.ds(pl.multiple_of(c * CSLOTS, CSLOTS), CSLOTS)
        msend[spot] = message.reshape(CSLOTS, 2, TILES * 128)
        send_chunk(c, msend, mrecv, ms_sem, mr_sem)
        return carry

    lax.fori_loop(0, CHUNKS, mix, 0)
    mrecv[SELF] = msend[SELF]

    perm_back = spot_of(-1)
    hot_d = jnp.concatenate(
        [jnp.where(dstv[i : i + 1, :] == node, 1.0, 0.0).astype(BF16) for i in range(2)], axis=1
    )
    hot_n = nt(hot_d, perm_back).astype(BF16)

    def unturn(c, carry):
        at = pl.ds(pl.multiple_of(c * CROWS, CROWS), CROWS)
        spot = pl.ds(pl.multiple_of(c * CSLOTS, CSLOTS), CSLOTS)
        wait_chunk(c, drecv, dr_sem)
        wait_chunk(c, mrecv, mr_sem)
        dtab[at, :] = drecv[spot].reshape(CROWS, 256).astype(F32)
        xs[at, 0 : TILES * 128] = mrecv[spot].reshape(CROWS, TILES * 128).astype(F32)
        sums = {}

        def flush(t):
            back[at, t * 128 : (t + 1) * 128] = sums.pop(t).astype(BF16)

        for l in DEGREES:
            spread = {}
            for a in range(-reach(l), reach(l) + 1):
                tile, half = PLACE[frame_slot(l, a)]
                got = xs[at, tile * 128 : (tile + 1) * 128]
                turned = pltpu.roll(got, 64, 1)
                spread[a] = jnp.where(low, got, turned) if half == 0 else jnp.where(low, turned, got)
            for t in tiles_of(l):
                for a in range(-reach(l), reach(l) + 1):
                    piece, _ = arranged(l, a)
                    tab = dtab[at, piece * 128 : (piece + 1) * 128]
                    term = pick(tab, pattern(lane, l, a, t)) * spread[a]
                    sums[t] = sums[t] + term if t in sums else term
                if not (l < 6 and t in tiles_of(l + 1)):
                    flush(t)
        return carry

    lax.fori_loop(0, CHUNKS, unturn, 0)

    square = jnp.zeros((64, 1), F32)
    for s in range(7):
        part = nn(hot_n, back[:, s * 448 : (s + 1) * 448])
        agg_ref[:, s * 448 : (s + 1) * 448] = part
        square = square + jnp.sum(part * part, axis=1, keepdims=True)
    sqs[...] = jnp.broadcast_to(square, (64, 128))
    swap = pltpu.make_async_remote_copy(
        src_ref=sqs,
        dst_ref=sqr,
        send_sem=q_sem.at[0],
        recv_sem=q_sem.at[1],
        device_id={"rep": 1 - rep},
        device_id_type=MESH,
    )
    swap.start()
    for c in range(CHUNKS):
        to_peer(c).wait_send()
        wait_chunk(c, dsend, ds_sem)
        wait_chunk(c, msend, ms_sem)
    swap.wait()
    sq_ref[...] = sqs[...] + sqr[...]


def shards(node_features, src_node, dst_node, counts, rotation, w_zero, w_one, w_two, norm_gain):
    x = node_features.reshape(64, 3136)
    rt = rotation.transpose(0, 3, 2, 1).reshape(235, 2, 128)
    src = src_node.transpose(0, 2, 1).reshape(2, 128)
    dst = dst_node.transpose(0, 2, 1).reshape(2, 128)
    wz = w_zero.transpose(1, 2, 0).reshape(448, 896)
    w1 = w_one.reshape(2, 768, 384)
    w2 = w_two.transpose(0, 2, 3, 1).reshape(2, 320, 640)
    hbm = pl.BlockSpec(memory_space=pltpu.MemorySpace.HBM)
    vmem = pl.BlockSpec(memory_space=pltpu.VMEM)
    dma = pltpu.SemaphoreType.DMA
    agg, total = pl.pallas_call(
        kernel,
        out_shape=(
            jax.ShapeDtypeStruct((64, 3136), F32),
            jax.ShapeDtypeStruct((64, 128), F32),
        ),
        in_specs=[hbm] * 8,
        out_specs=(vmem, vmem),
        scratch_shapes=[
            pltpu.VMEM((64, 3136), BF16),
            pltpu.VMEM((235, 2, 128), BF16),
            pltpu.VMEM((2, 128), jnp.int32),
            pltpu.VMEM((2, 128), jnp.int32),
            pltpu.VMEM((1, 128), jnp.int32),
            pltpu.VMEM((448, 896), BF16),
            pltpu.VMEM((2, 768, 384), BF16),
            pltpu.VMEM((2, 320, 640), BF16),
            pltpu.VMEM((256, 256), F32),
            pltpu.VMEM((ROWS, 256), F32),
            pltpu.VMEM((ROWS, 3200), F32),
            pltpu.VMEM((ROWS, 29 * 128), BF16),
            pltpu.VMEM((ROWS, TILES * 128), BF16),
            pltpu.VMEM((ROWS, TILES * 128), BF16),
            pltpu.VMEM((CROWS, 29 * 128), BF16),
            pltpu.VMEM((SLOTS, 2, TILES * 128), BF16),
            pltpu.VMEM((SLOTS, 2, TILES * 128), BF16),
            pltpu.VMEM((SLOTS, 2, 256), BF16),
            pltpu.VMEM((SLOTS, 2, 256), BF16),
            pltpu.VMEM((ROWS, 3200), BF16),
            pltpu.VMEM((64, 128), F32),
            pltpu.VMEM((64, 128), F32),
            dma((8,)),
            dma((CHUNKS,)),
            dma((CHUNKS,)),
            dma((CHUNKS,)),
            dma((CHUNKS,)),
            dma((CHUNKS,)),
            dma((CHUNKS,)),
            dma((2,)),
        ],
        compiler_params=pltpu.CompilerParams(
            collective_id=0, has_side_effects=True, vmem_limit_bytes=48 * 2**20
        ),
    )(x, rt, src, dst, counts, wz, w1, w2)
    scale = lax.rsqrt(total[:, 0:1] / 6272.0 + 1e-06)
    updated = x.astype(F32) + norm_gain * (agg * scale)
    return updated.astype(BF16).reshape(64, 1, 3136)


def solution(mesh):
    return jax.shard_map(
        shards,
        mesh=mesh,
        in_specs=(
            P("dev", "rep", None),
            P("dev", None, None),
            P("dev", None, None),
            P("dev", None),
            P("dev", None, None, None),
            P(None, "rep", None),
            P(None, None, "rep", None),
            P(None, None, "rep", None),
            P("rep", None),
        ),
        out_specs=P("dev", "rep", None),
        check_vma=False,
    )
```

```python
import functools

import jax
import jax.numpy as jnp
from jax import lax
from jax.experimental import pallas as pl
from jax.experimental.pallas import tpu as pltpu
from jax.sharding import PartitionSpec as P

MESH = pl.DeviceIdType.MESH
F32 = jnp.float32
BF16 = jnp.bfloat16

SLOTS = 128
ROWS = 256
CHUNKS = 2
CROWS = ROWS // CHUNKS
CSLOTS = SLOTS // CHUNKS
SELF = 7
TILES = 15
WIDTH = 3136
DEGREES = range(7)


def reach(l):
    return min(l, 2)


def orders(l):
    return range(-reach(l), reach(l) + 1)


def frame_slot(degree, order):
    if order == 0:
        return degree
    if order == 1:
        return 6 + degree
    if order == -1:
        return 12 + degree
    if order == 2:
        return 17 + degree
    return 22 + degree


def entry(l, a, b):
    start = sum((2 * m + 1) * (2 * reach(m) + 1) for m in range(l))
    return start + (a + reach(l)) * (2 * l + 1) + b + l


def message_places():
    place = {}
    for r in range(6):
        place[r] = (r // 2, r % 2)
    for r in range(7, 19):
        place[r] = (3 + (r - 7) // 2, (r - 7) % 2)
    for r in range(19, 23):
        place[r] = (9 + (r - 19) // 2, (r - 19) % 2)
    for r in range(24, 28):
        place[r] = (11 + (r - 24) // 2, (r - 24) % 2)
    place[23] = (13, 0)
    place[28] = (13, 1)
    place[6] = (14, 0)
    return place


PLACE = message_places()


def nt(a, b):
    return lax.dot_general(a, b, (((1,), (1,)), ((), ())), preferred_element_type=F32)


def nn(a, b):
    return jnp.dot(a, b, preferred_element_type=F32)


def z_step(k):
    return [4, 3, 5, 2, 6, 1, 7, 0][k]


def unit(n):
    rows = lax.broadcasted_iota(jnp.int32, (n, n), 0)
    cols = lax.broadcasted_iota(jnp.int32, (n, n), 1)
    return jnp.where(rows == cols, 1.0, 0.0).astype(BF16)


def kernel(
    x_hbm, rt_hbm, src_hbm, dst_hbm, cnt_hbm, wz_hbm, w1_hbm, w2_hbm, gain_hbm,
    out_ref,
    xv, rtv, srcv, dstv, cntv, wz, w1, w2, gain,
    rts, dtab, xs, rot, msend, mrecv, dsend, drecv, back, agg, sqs, sqr,
    load_sem, ps_sem, pr_sem, ms_sem, mr_sem, ds_sem, dr_sem, q_sem,
):
    me = lax.axis_index("dev")
    rep = lax.axis_index("rep")
    px, pz, py = me // 32, (me // 4) % 8, me % 4
    barrier = pltpu.get_barrier_semaphore()

    loads = [
        pltpu.make_async_copy(s, d, load_sem.at[i])
        for i, (s, d) in enumerate(
            [
                (rt_hbm, rtv), (src_hbm, srcv), (dst_hbm, dstv), (cnt_hbm, cntv), (x_hbm, xv),
                (wz_hbm, wz), (w1_hbm, w1), (w2_hbm, w2), (gain_hbm, gain),
            ]
        )
    ]
    for copy in loads:
        copy.start()

    def greet(g, carry):
        for k in range(8):
            pl.semaphore_signal(
                barrier, inc=1, device_id={"dev": (me + g * 8 + k + 1) % SLOTS}, device_id_type=MESH
            )
        return carry

    lax.fori_loop(0, 15, greet, 0)
    for k in range(121, SLOTS):
        pl.semaphore_signal(barrier, inc=1, device_id={"dev": (me + k) % SLOTS}, device_id_type=MESH)
    pl.semaphore_signal(barrier, inc=1, device_id={"rep": 1 - rep}, device_id_type=MESH)

    def spot_of(sign):
        q = lax.broadcasted_iota(jnp.int32, (ROWS, 128), 0)
        col = lax.broadcasted_iota(jnp.int32, (ROWS, 128), 1)
        slot, i = q >> 1, q & 1
        k, r = slot & 7, slot >> 3
        h = (k + 1) >> 1
        oz = jnp.where((k & 1) == 1, 4 - h, 4 + h)
        ox = r >> 2
        oy = r + ox
        tx = (px + sign * ox + 8) & 3
        tz = (pz + sign * oz + 16) & 7
        ty = (py + sign * oy + 32) & 3
        target = tx * 32 + tz * 4 + ty
        hit = jnp.where(col == target, 1, 0)
        return jnp.concatenate(
            [jnp.where(i == side, hit, 0).astype(F32).astype(BF16) for side in range(2)], axis=1
        )

    perm = spot_of(1)
    eye = unit(128)
    node = lax.broadcasted_iota(jnp.int32, (64, 128), 0)

    for copy in loads[:5]:
        copy.wait()
    hot = jnp.concatenate(
        [
            jnp.where((srcv[i : i + 1, :] == node) & (cntv[0:1, :] > i), 1.0, 0.0).astype(BF16)
            for i in range(2)
        ],
        axis=1,
    )
    hot_q = nt(hot, perm).astype(BF16)
    for t in range(25):
        wide = 128 if t < 24 else 64
        turned = nt(eye[0:wide, 0:wide], xv[:, t * 128 : t * 128 + wide]).astype(BF16)
        xs[t * 128 : t * 128 + wide, :] = nn(turned, hot_q)

    rts[...] = jnp.zeros_like(rts)
    for i in range(2):
        rts[0:235, i * 128 : (i + 1) * 128] = rtv[:, i, :].astype(F32)
    table = rts[...].astype(BF16)
    dtab[...] = nt(table, perm)
    dsend[...] = nt(perm, table).astype(BF16).reshape(SLOTS, 2, 256)

    def lanes(c):
        return slice(c * 128, (c + 1) * 128)

    def turn(c):
        at = lanes(c)
        for l in DEGREES:
            sums = {}
            for b in range(-l, l + 1):
                k = l * l + l + b
                part = xs[k * 64 : (k + 1) * 64, at]
                for a in orders(l):
                    e = entry(l, a, b)
                    term = dtab[e : e + 1, at] * part
                    sums[a] = sums[a] + term if a in sums else term
            for a in orders(l):
                rot[c, frame_slot(l, a), rep] = sums[a].astype(BF16)

    def to_peer(c):
        return pltpu.make_async_remote_copy(
            src_ref=rot.at[c, :, rep],
            dst_ref=rot.at[c, :, rep],
            send_sem=ps_sem.at[c],
            recv_sem=pr_sem.at[c],
            device_id={"rep": 1 - rep},
            device_id_type=MESH,
        )

    tz = [(pz + z_step(k)) % 8 for k in range(8)]

    def send_chunk(c, source, target, send_sem, recv_sem):
        def group(g, carry):
            r = c * (CSLOTS // 8) + g
            tx = (px + r // 4) % 4
            ty = (py + r + r // 4) % 4
            for k in range(8):
                slot = r * 8 + k
                copy = pltpu.make_async_remote_copy(
                    src_ref=source.at[slot],
                    dst_ref=target.at[slot],
                    send_sem=send_sem.at[c],
                    recv_sem=recv_sem.at[c],
                    device_id={"dev": (tx * 8 + tz[k]) * 4 + ty},
                    device_id_type=MESH,
                )
                if k == SELF and c == 0:

                    @pl.when(r > 0)
                    def _():
                        copy.start()
                else:
                    copy.start()
            return carry

        lax.fori_loop(0, CSLOTS // 8, group, 0)

    def wait_chunk(c, buffer, sem):
        part = buffer.at[pl.ds(c * CSLOTS, CSLOTS - 1 if c == 0 else CSLOTS)]
        pltpu.make_async_copy(part, part, sem.at[c]).wait()

    def mix(c):
        to_peer(c).wait_recv()

        def rows(first, count):
            part = rot[c, first : first + count].reshape(count * 128, 128)
            return nt(eye, part).astype(BF16)

        zero = nt(rows(0, 7), wz[...])
        one = jnp.concatenate([rows(7, 6), rows(13, 6)], axis=0)
        two = jnp.concatenate([rows(19, 5), rows(24, 5)], axis=0)
        first, second = nn(one, w1[0]), nn(one, w1[1])
        plus1 = first[0:128] - second[128:256]
        minus1 = second[0:128] + first[128:256]
        first, second = nt(two, w2[0]), nt(two, w2[1])
        plus2 = first[0:128] - second[128:256]
        minus2 = second[0:128] + first[128:256]
        last = jnp.concatenate([plus2[:, 256:320], minus2[:, 256:320]], axis=1)
        tail = jnp.concatenate([zero[:, 384:448], jnp.zeros((CROWS, 64), F32)], axis=1)
        pieces = [zero[:, 0:384], plus1, minus1, plus2[:, 0:256], minus2[:, 0:256], last, tail]
        spot = 0
        for piece in pieces:
            wide = piece.shape[1]
            msend[c * CSLOTS : (c + 1) * CSLOTS, :, spot : spot + wide] = piece.astype(BF16).reshape(
                CSLOTS, 2, wide
            )
            spot += wide

    def unturn(c):
        at = lanes(c)
        wait_chunk(c, drecv, dr_sem)
        if c == 0:
            drecv[SELF] = dsend[SELF]
        rows = drecv[c * CSLOTS : (c + 1) * CSLOTS].reshape(CROWS, 256)
        dtab[0:128, at] = nt(eye, rows[:, 0:128])
        dtab[128:256, at] = nt(eye, rows[:, 128:256])
        wait_chunk(c, mrecv, mr_sem)
        if c == 0:
            mrecv[SELF] = msend[SELF]
        for t in range(TILES):
            tile = mrecv[c * CSLOTS : (c + 1) * CSLOTS, :, t * 128 : (t + 1) * 128].reshape(CROWS, 128)
            xs[t * 128 : (t + 1) * 128, at] = nt(eye, tile)
        for l in DEGREES:
            parts = {}
            for a in orders(l):
                tile, half = PLACE[frame_slot(l, a)]
                spot = (2 * tile + half) * 64
                parts[a] = xs[spot : spot + 64, at]
            for b in range(-l, l + 1):
                total = None
                for a in orders(l):
                    e = entry(l, a, b)
                    term = dtab[e : e + 1, at] * parts[a]
                    total = term if total is None else total + term
                k = l * l + l + b
                back[k * 64 : (k + 1) * 64, at] = total.astype(BF16)

    for c in range(CHUNKS):
        turn(c)

    pl.semaphore_wait(barrier, SLOTS)
    for c in range(CHUNKS):
        to_peer(c).start()
    for c in range(CHUNKS):
        send_chunk(c, dsend, drecv, ds_sem, dr_sem)

    for copy in loads[5:]:
        copy.wait()
    for c in range(CHUNKS):
        mix(c)
        send_chunk(c, msend, mrecv, ms_sem, mr_sem)

    perm_back = spot_of(-1)
    hot_d = jnp.concatenate(
        [jnp.where(dstv[i : i + 1, :] == node, 1.0, 0.0).astype(BF16) for i in range(2)], axis=1
    )
    hot_n = nt(hot_d, perm_back).astype(BF16)

    for c in range(CHUNKS):
        unturn(c)

    square = jnp.zeros((64, 1), F32)
    for s in range(7):
        at = slice(s * 448, (s + 1) * 448)
        part = nt(hot_n, back[at, :])
        agg[:, at] = part
        square = square + jnp.sum(part * part, axis=1, keepdims=True)
    sqs[...] = jnp.broadcast_to(square, (64, 128))
    swap = pltpu.make_async_remote_copy(
        src_ref=sqs,
        dst_ref=sqr,
        send_sem=q_sem.at[0],
        recv_sem=q_sem.at[1],
        device_id={"rep": 1 - rep},
        device_id_type=MESH,
    )
    swap.start()
    for c in range(CHUNKS):
        to_peer(c).wait_send()
        wait_chunk(c, dsend, ds_sem)
        wait_chunk(c, msend, ms_sem)
    swap.wait()
    mean = (sqs[...] + sqr[...]) / 6272.0
    scale = lax.rsqrt(mean + 1e-06)[:, 0:1]
    for s in range(7):
        at = slice(s * 448, (s + 1) * 448)
        normed = agg[:, at] * scale
        out_ref[:, at] = (xv[:, at].astype(F32) + gain[0:1, at] * normed).astype(BF16)


def shards(node_features, src_node, dst_node, counts, rotation, w_zero, w_one, w_two, norm_gain):
    x = node_features.reshape(64, WIDTH)
    rt = rotation.transpose(0, 3, 2, 1).reshape(235, 2, 128)
    src = src_node.transpose(0, 2, 1).reshape(2, 128)
    dst = dst_node.transpose(0, 2, 1).reshape(2, 128)
    wz = w_zero.transpose(1, 2, 0).reshape(448, 896)
    w1 = w_one.reshape(2, 768, 384)
    w2 = w_two.transpose(0, 2, 3, 1).reshape(2, 320, 640)
    hbm = pl.BlockSpec(memory_space=pltpu.MemorySpace.HBM)
    vmem = pl.BlockSpec(memory_space=pltpu.VMEM)
    dma = pltpu.SemaphoreType.DMA
    updated = pl.pallas_call(
        kernel,
        out_shape=jax.ShapeDtypeStruct((64, WIDTH), BF16),
        in_specs=[hbm] * 9,
        out_specs=vmem,
        scratch_shapes=[
            pltpu.VMEM((64, WIDTH), BF16),
            pltpu.VMEM((235, 2, 128), BF16),
            pltpu.VMEM((2, 128), jnp.int32),
            pltpu.VMEM((2, 128), jnp.int32),
            pltpu.VMEM((1, 128), jnp.int32),
            pltpu.VMEM((448, 896), BF16),
            pltpu.VMEM((2, 768, 384), BF16),
            pltpu.VMEM((2, 320, 640), BF16),
            pltpu.VMEM((1, WIDTH), F32),
            pltpu.VMEM((256, 256), F32),
            pltpu.VMEM((256, ROWS), F32),
            pltpu.VMEM((WIDTH, ROWS), F32),
            pltpu.VMEM((CHUNKS, 29, 2, 64, 128), BF16),
            pltpu.VMEM((SLOTS, 2, TILES * 128), BF16),
            pltpu.VMEM((SLOTS, 2, TILES * 128), BF16),
            pltpu.VMEM((SLOTS, 2, 256), BF16),
            pltpu.VMEM((SLOTS, 2, 256), BF16),
            pltpu.VMEM((WIDTH, ROWS), BF16),
            pltpu.VMEM((64, WIDTH), F32),
            pltpu.VMEM((64, 128), F32),
            pltpu.VMEM((64, 128), F32),
            dma((9,)),
            dma((CHUNKS,)),
            dma((CHUNKS,)),
            dma((CHUNKS,)),
            dma((CHUNKS,)),
            dma((CHUNKS,)),
            dma((CHUNKS,)),
            dma((2,)),
        ],
        compiler_params=pltpu.CompilerParams(
            collective_id=0, has_side_effects=True, vmem_limit_bytes=67043328
        ),
    )(x, rt, src, dst, counts, wz, w1, w2, norm_gain)
    return updated.reshape(64, 1, WIDTH)


def solution(mesh):
    return jax.shard_map(
        shards,
        mesh=mesh,
        in_specs=(
            P("dev", "rep", None),
            P("dev", None, None),
            P("dev", None, None),
            P("dev", None),
            P("dev", None, None, None),
            P(None, "rep", None),
            P(None, None, "rep", None),
            P(None, None, "rep", None),
            P("rep", None),
        ),
        out_specs=P("dev", "rep", None),
        check_vma=False,
    )
```

```python
import functools

import jax
import jax.numpy as jnp
from jax import lax
from jax.experimental import pallas as pl
from jax.experimental.pallas import tpu as pltpu
from jax.sharding import PartitionSpec as P

MESH = pl.DeviceIdType.MESH
F32 = jnp.float32
BF16 = jnp.bfloat16

SLOTS = 128
ROWS = 256
CHUNKS = 2
CROWS = ROWS // CHUNKS
CSLOTS = SLOTS // CHUNKS
TILES = 15
WIDTH = 3136
LEAD = ((0, 1), (1, 3), (2, 4))
DEGREES = range(7)


def reach(l):
    return min(l, 2)


def orders(l):
    return range(-reach(l), reach(l) + 1)


def frame_slot(degree, order):
    if order == 0:
        return degree
    if order == 1:
        return 6 + degree
    if order == -1:
        return 12 + degree
    if order == 2:
        return 17 + degree
    return 22 + degree


def entry(l, a, b):
    start = sum((2 * m + 1) * (2 * reach(m) + 1) for m in range(l))
    return start + (a + reach(l)) * (2 * l + 1) + b + l


def message_places():
    place = {}
    for r in range(6):
        place[r] = (r // 2, r % 2)
    for r in range(7, 19):
        place[r] = (3 + (r - 7) // 2, (r - 7) % 2)
    for r in range(19, 23):
        place[r] = (9 + (r - 19) // 2, (r - 19) % 2)
    for r in range(24, 28):
        place[r] = (11 + (r - 24) // 2, (r - 24) % 2)
    place[23] = (13, 0)
    place[28] = (13, 1)
    place[6] = (14, 0)
    return place


PLACE = message_places()


def nt(a, b):
    return lax.dot_general(a, b, (((1,), (1,)), ((), ())), preferred_element_type=F32)


def nn(a, b):
    return jnp.dot(a, b, preferred_element_type=F32)


def unit(n):
    rows = lax.broadcasted_iota(jnp.int32, (n, n), 0)
    cols = lax.broadcasted_iota(jnp.int32, (n, n), 1)
    return jnp.where(rows == cols, 1.0, 0.0).astype(BF16)


def kernel(
    x_hbm, rt_hbm, src_hbm, dst_hbm, cnt_hbm, wz_hbm, w1_hbm, w2_hbm, gain_hbm,
    out_ref,
    xv, rtv, srcv, dstv, cntv, wz, w1, w2, gain,
    rts, dtab, xs, rot, msend, mrecv, dsend, drecv, back, agg, sqs, sqr,
    load_sem, ps_sem, pr_sem, ms_sem, mr_sem, ds_sem, dr_sem, q_sem,
):
    me = lax.axis_index("dev")
    rep = lax.axis_index("rep")
    px, pz, py = me // 32, (me // 4) % 8, me % 4
    barrier = pltpu.get_barrier_semaphore()

    loads = [
        pltpu.make_async_copy(s, d, load_sem.at[i])
        for i, (s, d) in enumerate(
            [
                (rt_hbm, rtv), (src_hbm, srcv), (dst_hbm, dstv), (cnt_hbm, cntv), (x_hbm, xv),
                (wz_hbm, wz), (w1_hbm, w1), (w2_hbm, w2), (gain_hbm, gain),
            ]
        )
    ]
    for copy in loads:
        copy.start()

    def greet(g, carry):
        for k in range(8):
            pl.semaphore_signal(
                barrier, inc=1, device_id={"dev": (me + g * 8 + k + 1) % SLOTS}, device_id_type=MESH
            )
        return carry

    lax.fori_loop(0, 15, greet, 0)
    for k in range(121, SLOTS):
        pl.semaphore_signal(barrier, inc=1, device_id={"dev": (me + k) % SLOTS}, device_id_type=MESH)
    pl.semaphore_signal(barrier, inc=1, device_id={"rep": 1 - rep}, device_id_type=MESH)

    def spot_of(sign):
        q = lax.broadcasted_iota(jnp.int32, (ROWS, 128), 0)
        col = lax.broadcasted_iota(jnp.int32, (ROWS, 128), 1)
        slot, i = q >> 1, q & 1
        oz, r = slot & 7, slot >> 3
        ox = r >> 2
        oy = r + ox
        tx = (px + sign * ox + 8) & 3
        tz = (pz + sign * oz + 16) & 7
        ty = (py + sign * oy + 32) & 3
        target = tx * 32 + tz * 4 + ty
        hit = jnp.where(col == target, 1, 0)
        return jnp.concatenate(
            [jnp.where(i == side, hit, 0).astype(F32).astype(BF16) for side in range(2)], axis=1
        )

    perm = spot_of(1)
    eye = unit(128)
    node = lax.broadcasted_iota(jnp.int32, (64, 128), 0)

    for copy in loads[:5]:
        copy.wait()
    hot = jnp.concatenate(
        [
            jnp.where((srcv[i : i + 1, :] == node) & (cntv[0:1, :] > i), 1.0, 0.0).astype(BF16)
            for i in range(2)
        ],
        axis=1,
    )
    hot_q = nt(hot, perm).astype(BF16)
    for t in range(25):
        wide = 128 if t < 24 else 64
        turned = nt(eye[0:wide, 0:wide], xv[:, t * 128 : t * 128 + wide]).astype(BF16)
        xs[t * 128 : t * 128 + wide, :] = nn(turned, hot_q)

    rts[...] = jnp.zeros_like(rts)
    for i in range(2):
        rts[0:235, i * 128 : (i + 1) * 128] = rtv[:, i, :].astype(F32)
    table = rts[...].astype(BF16)
    dtab[...] = nt(table, perm)
    dsend[...] = nt(perm, table).astype(BF16).reshape(SLOTS, 2, 256)

    def lanes(c):
        return slice(c * 128, (c + 1) * 128)

    def turn(c):
        at = lanes(c)
        for l in DEGREES:
            sums = {}
            for b in range(-l, l + 1):
                k = l * l + l + b
                part = xs[k * 64 : (k + 1) * 64, at]
                for a in orders(l):
                    e = entry(l, a, b)
                    term = dtab[e : e + 1, at] * part
                    sums[a] = sums[a] + term if a in sums else term
            for a in orders(l):
                rot[c, frame_slot(l, a), rep] = sums[a].astype(BF16)

    def to_peer(c):
        return pltpu.make_async_remote_copy(
            src_ref=rot.at[c, :, rep],
            dst_ref=rot.at[c, :, rep],
            send_sem=ps_sem.at[c],
            recv_sem=pr_sem.at[c],
            device_id={"rep": 1 - rep},
            device_id_type=MESH,
        )

    def send(r, plane, allowed, source, target, send_sem, recv_sem):
        tx = (px + (r >> 2)) & 3
        ty = (py + r + (r >> 2)) & 3
        slot = r * 8 + ((plane - pz) & 7)
        copy = pltpu.make_async_remote_copy(
            src_ref=source.at[slot],
            dst_ref=target.at[slot],
            send_sem=send_sem.at[r >> 3],
            recv_sem=recv_sem.at[r >> 3],
            device_id={"dev": tx * 32 + plane * 4 + ty},
            device_id_type=MESH,
        )

        @pl.when(allowed & (slot > 0))
        def _():
            copy.start()

    planes = [(pz + step) & 7 for step in (4, 3, 5, 2, 6, 1, 7, 0)]

    def send_steps(first, last, buffers, lead):
        def step(t, carry):
            for plane in planes:
                r = t
                for early, gap in lead:
                    r = r + jnp.where(plane == early, t // gap, 0)
                send(r, plane, r < 16, *buffers)
            for early, gap in lead:
                r = t + t // gap + 1
                send(r, early, (t % gap == gap - 1) & (r < 16), *buffers)
            return carry

        lax.fori_loop(first, last, step, 0)

    def wait_chunk(c, buffer, sem):
        part = buffer.at[pl.ds(c * CSLOTS, CSLOTS - 1 if c == 0 else CSLOTS)]
        pltpu.make_async_copy(part, part, sem.at[c]).wait()

    def mix(c):
        to_peer(c).wait_recv()

        def rows(first, count):
            part = rot[c, first : first + count].reshape(count * 128, 128)
            return nt(eye, part).astype(BF16)

        zero = nt(rows(0, 7), wz[...])
        one = jnp.concatenate([rows(7, 6), rows(13, 6)], axis=0)
        two = jnp.concatenate([rows(19, 5), rows(24, 5)], axis=0)
        first, second = nn(one, w1[0]), nn(one, w1[1])
        plus1 = first[0:128] - second[128:256]
        minus1 = second[0:128] + first[128:256]
        first, second = nt(two, w2[0]), nt(two, w2[1])
        plus2 = first[0:128] - second[128:256]
        minus2 = second[0:128] + first[128:256]
        last = jnp.concatenate([plus2[:, 256:320], minus2[:, 256:320]], axis=1)
        tail = jnp.concatenate([zero[:, 384:448], jnp.zeros((CROWS, 64), F32)], axis=1)
        pieces = [zero[:, 0:384], plus1, minus1, plus2[:, 0:256], minus2[:, 0:256], last, tail]
        spot = 0
        for piece in pieces:
            wide = piece.shape[1]
            msend[c * CSLOTS : (c + 1) * CSLOTS, :, spot : spot + wide] = piece.astype(BF16).reshape(
                CSLOTS, 2, wide
            )
            spot += wide

    def unturn(c):
        at = lanes(c)
        wait_chunk(c, drecv, dr_sem)
        if c == 0:
            drecv[0] = dsend[0]
        rows = drecv[c * CSLOTS : (c + 1) * CSLOTS].reshape(CROWS, 256)
        dtab[0:128, at] = nt(eye, rows[:, 0:128])
        dtab[128:256, at] = nt(eye, rows[:, 128:256])
        wait_chunk(c, mrecv, mr_sem)
        if c == 0:
            mrecv[0] = msend[0]
        for t in range(TILES):
            tile = mrecv[c * CSLOTS : (c + 1) * CSLOTS, :, t * 128 : (t + 1) * 128].reshape(CROWS, 128)
            xs[t * 128 : (t + 1) * 128, at] = nt(eye, tile)
        for l in DEGREES:
            parts = {}
            for a in orders(l):
                tile, half = PLACE[frame_slot(l, a)]
                spot = (2 * tile + half) * 64
                parts[a] = xs[spot : spot + 64, at]
            for b in range(-l, l + 1):
                total = None
                for a in orders(l):
                    e = entry(l, a, b)
                    term = dtab[e : e + 1, at] * parts[a]
                    total = term if total is None else total + term
                k = l * l + l + b
                back[k * 64 : (k + 1) * 64, at] = total.astype(BF16)

    for c in range(CHUNKS):
        turn(c)

    pl.semaphore_wait(barrier, SLOTS)
    for c in range(CHUNKS):
        to_peer(c).start()
    send_steps(0, 16, (dsend, drecv, ds_sem, dr_sem), ())

    for copy in loads[5:]:
        copy.wait()
    mix(0)
    send_steps(0, 4, (msend, mrecv, ms_sem, mr_sem), LEAD)
    mix(1)
    send_steps(4, 16, (msend, mrecv, ms_sem, mr_sem), LEAD)

    perm_back = spot_of(-1)
    hot_d = jnp.concatenate(
        [jnp.where(dstv[i : i + 1, :] == node, 1.0, 0.0).astype(BF16) for i in range(2)], axis=1
    )
    hot_n = nt(hot_d, perm_back).astype(BF16)

    square = jnp.zeros((64, 1), F32)
    for c in range(CHUNKS):
        unturn(c)
        for s in range(7):
            at = slice(s * 448, (s + 1) * 448)
            part = nt(hot_n[:, lanes(c)], back[at, lanes(c)])
            if c > 0:
                part = agg[:, at] + part
            agg[:, at] = part
            if c == CHUNKS - 1:
                square = square + jnp.sum(part * part, axis=1, keepdims=True)
    sqs[...] = jnp.broadcast_to(square, (64, 128))
    swap = pltpu.make_async_remote_copy(
        src_ref=sqs,
        dst_ref=sqr,
        send_sem=q_sem.at[0],
        recv_sem=q_sem.at[1],
        device_id={"rep": 1 - rep},
        device_id_type=MESH,
    )
    swap.start()
    for c in range(CHUNKS):
        to_peer(c).wait_send()
        wait_chunk(c, dsend, ds_sem)
        wait_chunk(c, msend, ms_sem)
    swap.wait()
    mean = (sqs[...] + sqr[...]) / 6272.0
    scale = lax.rsqrt(mean + 1e-06)[:, 0:1]
    for s in range(7):
        at = slice(s * 448, (s + 1) * 448)
        normed = agg[:, at] * scale
        out_ref[:, at] = (xv[:, at].astype(F32) + gain[0:1, at] * normed).astype(BF16)


def shards(node_features, src_node, dst_node, counts, rotation, w_zero, w_one, w_two, norm_gain):
    x = node_features.reshape(64, WIDTH)
    rt = rotation.transpose(0, 3, 2, 1).reshape(235, 2, 128)
    src = src_node.transpose(0, 2, 1).reshape(2, 128)
    dst = dst_node.transpose(0, 2, 1).reshape(2, 128)
    wz = w_zero.transpose(1, 2, 0).reshape(448, 896)
    w1 = w_one.reshape(2, 768, 384)
    w2 = w_two.transpose(0, 2, 3, 1).reshape(2, 320, 640)
    hbm = pl.BlockSpec(memory_space=pltpu.MemorySpace.HBM)
    vmem = pl.BlockSpec(memory_space=pltpu.VMEM)
    dma = pltpu.SemaphoreType.DMA
    updated = pl.pallas_call(
        kernel,
        out_shape=jax.ShapeDtypeStruct((64, WIDTH), BF16),
        in_specs=[hbm] * 9,
        out_specs=vmem,
        scratch_shapes=[
            pltpu.VMEM((64, WIDTH), BF16),
            pltpu.VMEM((235, 2, 128), BF16),
            pltpu.VMEM((2, 128), jnp.int32),
            pltpu.VMEM((2, 128), jnp.int32),
            pltpu.VMEM((1, 128), jnp.int32),
            pltpu.VMEM((448, 896), BF16),
            pltpu.VMEM((2, 768, 384), BF16),
            pltpu.VMEM((2, 320, 640), BF16),
            pltpu.VMEM((1, WIDTH), F32),
            pltpu.VMEM((256, 256), F32),
            pltpu.VMEM((256, ROWS), F32),
            pltpu.VMEM((WIDTH, ROWS), F32),
            pltpu.VMEM((CHUNKS, 29, 2, 64, 128), BF16),
            pltpu.VMEM((SLOTS, 2, TILES * 128), BF16),
            pltpu.VMEM((SLOTS, 2, TILES * 128), BF16),
            pltpu.VMEM((SLOTS, 2, 256), BF16),
            pltpu.VMEM((SLOTS, 2, 256), BF16),
            pltpu.VMEM((WIDTH, ROWS), BF16),
            pltpu.VMEM((64, WIDTH), F32),
            pltpu.VMEM((64, 128), F32),
            pltpu.VMEM((64, 128), F32),
            dma((9,)),
            dma((CHUNKS,)),
            dma((CHUNKS,)),
            dma((CHUNKS,)),
            dma((CHUNKS,)),
            dma((CHUNKS,)),
            dma((CHUNKS,)),
            dma((2,)),
        ],
        compiler_params=pltpu.CompilerParams(
            collective_id=0, has_side_effects=True, vmem_limit_bytes=40000000
        ),
    )(*[pltpu.with_memory_space_constraint(v, pltpu.MemorySpace.HBM) for v in (x, rt, src, dst, counts, wz, w1, w2, norm_gain)])
    return updated.reshape(64, 1, WIDTH)


def solution(mesh):
    return jax.shard_map(
        shards,
        mesh=mesh,
        in_specs=(
            P("dev", "rep", None),
            P("dev", None, None),
            P("dev", None, None),
            P("dev", None),
            P("dev", None, None, None),
            P(None, "rep", None),
            P(None, None, "rep", None),
            P(None, None, "rep", None),
            P("rep", None),
        ),
        out_specs=P("dev", "rep", None),
        check_vma=False,
    )
```

```python
import functools

import jax
import jax.numpy as jnp
from jax import lax
from jax.experimental import pallas as pl
from jax.experimental.pallas import tpu as pltpu
from jax.sharding import PartitionSpec as P

MESH = pl.DeviceIdType.MESH
F32 = jnp.float32
BF16 = jnp.bfloat16

SLOTS = 128
ROWS = 256
CHUNKS = 2
CROWS = ROWS // CHUNKS
CSLOTS = SLOTS // CHUNKS
ZERO_TILES = 4
REST_TILES = 11
TILES = ZERO_TILES + REST_TILES
WIDTH = 3136
LEAD = ((0, 1), (1, 2), (2, 3), (3, 6))
DEGREES = range(7)


def reach(l):
    return min(l, 2)


def orders(l):
    return range(-reach(l), reach(l) + 1)


def frame_slot(degree, order):
    if order == 0:
        return degree
    if order == 1:
        return 6 + degree
    if order == -1:
        return 12 + degree
    if order == 2:
        return 17 + degree
    return 22 + degree


def entry(l, a, b):
    start = sum((2 * m + 1) * (2 * reach(m) + 1) for m in range(l))
    return start + (a + reach(l)) * (2 * l + 1) + b + l


def message_places():
    place = {}
    for r in range(7):
        place[r] = (r // 2, r % 2)
    for r in range(7, 19):
        place[r] = (ZERO_TILES + (r - 7) // 2, (r - 7) % 2)
    for r in range(19, 23):
        place[r] = (ZERO_TILES + 6 + (r - 19) // 2, (r - 19) % 2)
    for r in range(24, 28):
        place[r] = (ZERO_TILES + 8 + (r - 24) // 2, (r - 24) % 2)
    place[23] = (ZERO_TILES + 10, 0)
    place[28] = (ZERO_TILES + 10, 1)
    return place


PLACE = message_places()


def nt(a, b):
    return lax.dot_general(a, b, (((1,), (1,)), ((), ())), preferred_element_type=F32)


def nn(a, b):
    return jnp.dot(a, b, preferred_element_type=F32)


def unit(n):
    rows = lax.broadcasted_iota(jnp.int32, (n, n), 0)
    cols = lax.broadcasted_iota(jnp.int32, (n, n), 1)
    return jnp.where(rows == cols, 1.0, 0.0).astype(BF16)


def kernel(
    x_hbm, rt_hbm, src_hbm, dst_hbm, cnt_hbm, wz_hbm, w1_hbm, w2_hbm, gain_hbm,
    out_ref,
    xv, rtv, srcv, dstv, cntv, wz, w1, w2, gain,
    rts, dtab, xs, rot, zsend, zrecv, msend, mrecv, dsend, drecv, dswap, back, agg, sqs, sqr,
    load_sem, ps_sem, pr_sem, zs_sem, zr_sem, ms_sem, mr_sem, ds_sem, dr_sem, ws_sem, wr_sem, q_sem,
):
    me = lax.axis_index("dev")
    rep = lax.axis_index("rep")
    px, pz, py = me // 32, (me // 4) % 8, me % 4
    barrier = pltpu.get_barrier_semaphore()

    def greet(g, carry):
        tx = (px + 2 + (g >> 2)) & 3
        ty = (py + 2 + g) & 3
        for step in (4, 3, 5, 2, 6, 1, 7):
            spot = tx * 32 + ((pz + step) & 7) * 4 + ty
            pl.semaphore_signal(barrier, inc=1, device_id={"dev": spot}, device_id_type=MESH)

        @pl.when(g != 10)
        def _():
            spot = tx * 32 + pz * 4 + ty
            pl.semaphore_signal(barrier, inc=1, device_id={"dev": spot}, device_id_type=MESH)

        return carry

    lax.fori_loop(0, 16, greet, 0)
    pl.semaphore_signal(barrier, inc=1, device_id={"rep": 1 - rep}, device_id_type=MESH)

    loads = [
        pltpu.make_async_copy(s, d, load_sem.at[i])
        for i, (s, d) in enumerate(
            [
                (rt_hbm, rtv), (src_hbm, srcv), (dst_hbm, dstv), (cnt_hbm, cntv), (x_hbm, xv),
                (wz_hbm, wz), (w1_hbm, w1), (w2_hbm, w2), (gain_hbm, gain),
            ]
        )
    ]
    for copy in loads:
        copy.start()

    def spot_of(sign):
        q = lax.broadcasted_iota(jnp.int32, (ROWS, 128), 0)
        col = lax.broadcasted_iota(jnp.int32, (ROWS, 128), 1)
        slot, i = q >> 1, q & 1
        oz, r = slot & 7, slot >> 3
        ox = r >> 2
        oy = r + ox
        tx = (px + sign * ox + 8) & 3
        tz = (pz + sign * oz + 16) & 7
        ty = (py + sign * oy + 32) & 3
        target = tx * 32 + tz * 4 + ty
        hit = jnp.where(col == target, 1, 0)
        return jnp.concatenate(
            [jnp.where(i == side, hit, 0).astype(F32).astype(BF16) for side in range(2)], axis=1
        )

    perm = spot_of(1)
    eye = unit(128)
    node = lax.broadcasted_iota(jnp.int32, (64, 128), 0)

    for copy in loads[:5]:
        copy.wait()
    hot = jnp.concatenate(
        [
            jnp.where((srcv[i : i + 1, :] == node) & (cntv[0:1, :] > i), 1.0, 0.0).astype(BF16)
            for i in range(2)
        ],
        axis=1,
    )
    hot_q = nt(hot, perm).astype(BF16)
    for t in range(25):
        wide = 128 if t < 24 else 64
        turned = nt(eye[0:wide, 0:wide], xv[:, t * 128 : t * 128 + wide]).astype(BF16)
        xs[t * 128 : t * 128 + wide, :] = nn(turned, hot_q)

    rts[...] = jnp.zeros_like(rts)
    for i in range(2):
        rts[0:235, i * 128 : (i + 1) * 128] = rtv[:, i, :].astype(F32)
    table = rts[...].astype(BF16)
    dtab[...] = nt(table, perm)
    half = rts[pl.ds(pl.multiple_of(rep * 128, 128), 128), :].astype(BF16)
    dsend[...] = nt(perm, half).astype(BF16).reshape(SLOTS, 2, 128)

    def lanes(c):
        return slice(c * 128, (c + 1) * 128)

    def turn(c, chosen):
        at = lanes(c)
        for l in DEGREES:
            wanted = [a for a in orders(l) if a in chosen]
            sums = {}
            for b in range(-l, l + 1):
                if wanted:
                    k = l * l + l + b
                    part = xs[k * 64 : (k + 1) * 64, at]
                for a in wanted:
                    e = entry(l, a, b)
                    term = dtab[e : e + 1, at] * part
                    sums[a] = sums[a] + term if a in sums else term
            for a in wanted:
                rot[c, frame_slot(l, a), rep] = sums[a].astype(BF16)

    def to_peer(c, part):
        rows = pl.ds(0, 7) if part == 0 else pl.ds(7, 22)
        return pltpu.make_async_remote_copy(
            src_ref=rot.at[c, rows, rep],
            dst_ref=rot.at[c, rows, rep],
            send_sem=ps_sem.at[c, part],
            recv_sem=pr_sem.at[c, part],
            device_id={"rep": 1 - rep},
            device_id_type=MESH,
        )

    def swap_table(c):
        return pltpu.make_async_remote_copy(
            src_ref=dswap.at[c, rep],
            dst_ref=dswap.at[c, rep],
            send_sem=ws_sem.at[c],
            recv_sem=wr_sem.at[c],
            device_id={"rep": 1 - rep},
            device_id_type=MESH,
        )

    def send(u, plane, allowed, ordered, source, target, send_sem, recv_sem):
        r = u
        if ordered:
            row = ((u & 7) >> 1) ^ ((u & 7) >> 2)
            ox = (u >> 3) * 2 + (u & 1)
            ahead = ox * 4 + ((row - py - ox) & 3)
            r = jnp.where(plane < 4, ahead, u)
        tx = (px + (r >> 2)) & 3
        ty = (py + r + (r >> 2)) & 3
        slot = r * 8 + ((plane - pz) & 7)
        copy = pltpu.make_async_remote_copy(
            src_ref=source.at[slot],
            dst_ref=target.at[slot],
            send_sem=send_sem.at[r >> 3],
            recv_sem=recv_sem.at[r >> 3],
            device_id={"dev": tx * 32 + plane * 4 + ty},
            device_id_type=MESH,
        )

        @pl.when(allowed & (slot > 0))
        def _():
            copy.start()

    planes = [(pz + step) & 7 for step in (4, 3, 5, 2, 6, 1, 7, 0)]

    def send_steps(first, last, buffers, lead):
        def step(t, carry):
            for plane in planes:
                r = t
                for early, gap in lead:
                    r = r + jnp.where(plane == early, t // gap, 0)
                send(r, plane, r < 16, bool(lead), *buffers)
            for early, gap in lead:
                r = t + t // gap + 1
                send(r, early, (t % gap == gap - 1) & (r < 16), True, *buffers)
            return carry

        lax.fori_loop(first, last, step, 0)

    def wait_chunk(c, buffer, sem):
        part = buffer.at[pl.ds(c * CSLOTS, CSLOTS - 1 if c == 0 else CSLOTS)]
        pltpu.make_async_copy(part, part, sem.at[c]).wait()

    def rows_of(c, first, count):
        part = rot[c, first : first + count].reshape(count * 128, 128)
        return nt(eye, part).astype(BF16)

    def mix_zero():
        for c in range(CHUNKS):
            to_peer(c, 0).wait_recv()
        zero = nt(jnp.concatenate([rows_of(c, 0, 7) for c in range(CHUNKS)], axis=0), wz[...])
        message = jnp.concatenate([zero, jnp.zeros((ROWS, 64), F32)], axis=1)
        zsend[...] = message.astype(BF16).reshape(SLOTS, 2, ZERO_TILES * 128)

    def mix(c):
        to_peer(c, 1).wait_recv()
        one = jnp.concatenate([rows_of(c, 7, 6), rows_of(c, 13, 6)], axis=0)
        two = jnp.concatenate([rows_of(c, 19, 5), rows_of(c, 24, 5)], axis=0)
        first, second = nn(one, w1[0]), nn(one, w1[1])
        plus1 = first[0:128] - second[128:256]
        minus1 = second[0:128] + first[128:256]
        first, second = nt(two, w2[0]), nt(two, w2[1])
        plus2 = first[0:128] - second[128:256]
        minus2 = second[0:128] + first[128:256]
        last = jnp.concatenate([plus2[:, 256:320], minus2[:, 256:320]], axis=1)
        spot = 0
        for piece in (plus1, minus1, plus2[:, 0:256], minus2[:, 0:256], last):
            wide = piece.shape[1]
            msend[c * CSLOTS : (c + 1) * CSLOTS, :, spot : spot + wide] = piece.astype(BF16).reshape(
                CSLOTS, 2, wide
            )
            spot += wide

    def table_in(c):
        wait_chunk(c, drecv, dr_sem)
        if c == 0:
            drecv[0] = dsend[0]
        rows = drecv[c * CSLOTS : (c + 1) * CSLOTS].reshape(CROWS, 128)
        dswap[c, rep] = nt(eye, rows).astype(BF16)
        swap_table(c).start()

    def tiles_in(c, buffer, count, first):
        for t in range(count):
            tile = buffer[c * CSLOTS : (c + 1) * CSLOTS, :, t * 128 : (t + 1) * 128].reshape(CROWS, 128)
            xs[(first + t) * 128 : (first + t + 1) * 128, lanes(c)] = nt(eye, tile)

    def zero_in(c):
        at = lanes(c)
        swap_table(c).wait_recv()
        dtab[0:128, at] = dswap[c, 0].astype(F32)
        dtab[128:256, at] = dswap[c, 1].astype(F32)
        wait_chunk(c, zrecv, zr_sem)
        if c == 0:
            zrecv[0] = zsend[0]
        tiles_in(c, zrecv, ZERO_TILES, 0)

    def unturn(c):
        at = lanes(c)
        wait_chunk(c, mrecv, mr_sem)
        if c == 0:
            mrecv[0] = msend[0]
        tiles_in(c, mrecv, REST_TILES, ZERO_TILES)
        for l in DEGREES:
            parts = {}
            for a in orders(l):
                tile, half = PLACE[frame_slot(l, a)]
                spot = (2 * tile + half) * 64
                parts[a] = xs[spot : spot + 64, at]
            for b in range(-l, l + 1):
                total = None
                for a in orders(l):
                    e = entry(l, a, b)
                    term = dtab[e : e + 1, at] * parts[a]
                    total = term if total is None else total + term
                k = l * l + l + b
                back[k * 64 : (k + 1) * 64, at] = total.astype(BF16)

    others = (-2, -1, 1, 2)
    for c in range(CHUNKS):
        turn(c, (0,))

    pl.semaphore_wait(barrier, SLOTS)
    for c in range(CHUNKS):
        to_peer(c, 0).start()
    send_steps(0, 16, (dsend, drecv, ds_sem, dr_sem), ())
    for c in range(CHUNKS):
        turn(c, others)
        to_peer(c, 1).start()

    for copy in loads[5:]:
        copy.wait()
    mix_zero()
    send_steps(0, 16, (zsend, zrecv, zs_sem, zr_sem), LEAD)
    mix(0)
    send_steps(0, 4, (msend, mrecv, ms_sem, mr_sem), LEAD)
    mix(1)
    send_steps(4, 16, (msend, mrecv, ms_sem, mr_sem), LEAD)

    perm_back = spot_of(-1)
    hot_d = jnp.concatenate(
        [jnp.where(dstv[i : i + 1, :] == node, 1.0, 0.0).astype(BF16) for i in range(2)], axis=1
    )
    hot_n = nt(hot_d, perm_back).astype(BF16)

    for c in range(CHUNKS):
        table_in(c)
    for c in range(CHUNKS):
        zero_in(c)
    square = jnp.zeros((64, 1), F32)
    for c in range(CHUNKS):
        unturn(c)
        for s in range(7):
            at = slice(s * 448, (s + 1) * 448)
            part = nt(hot_n[:, lanes(c)], back[at, lanes(c)])
            if c > 0:
                part = agg[:, at] + part
            agg[:, at] = part
            if c == CHUNKS - 1:
                square = square + jnp.sum(part * part, axis=1, keepdims=True)
    sqs[...] = jnp.broadcast_to(square, (64, 128))
    swap = pltpu.make_async_remote_copy(
        src_ref=sqs,
        dst_ref=sqr,
        send_sem=q_sem.at[0],
        recv_sem=q_sem.at[1],
        device_id={"rep": 1 - rep},
        device_id_type=MESH,
    )
    swap.start()
    for c in range(CHUNKS):
        to_peer(c, 0).wait_send()
        to_peer(c, 1).wait_send()
        swap_table(c).wait_send()
        wait_chunk(c, dsend, ds_sem)
        wait_chunk(c, zsend, zs_sem)
        wait_chunk(c, msend, ms_sem)
    swap.wait()
    mean = (sqs[...] + sqr[...]) / 6272.0
    scale = lax.rsqrt(mean + 1e-06)[:, 0:1]
    for s in range(7):
        at = slice(s * 448, (s + 1) * 448)
        normed = agg[:, at] * scale
        out_ref[:, at] = (xv[:, at].astype(F32) + gain[0:1, at] * normed).astype(BF16)


def shards(node_features, src_node, dst_node, counts, rotation, w_zero, w_one, w_two, norm_gain):
    x = node_features.reshape(64, WIDTH)
    rt = rotation.transpose(0, 3, 2, 1).reshape(235, 2, 128)
    src = src_node.transpose(0, 2, 1).reshape(2, 128)
    dst = dst_node.transpose(0, 2, 1).reshape(2, 128)
    wz = w_zero.transpose(1, 2, 0).reshape(448, 896)
    w1 = w_one.reshape(2, 768, 384)
    w2 = w_two.transpose(0, 2, 3, 1).reshape(2, 320, 640)
    hbm = pl.BlockSpec(memory_space=pltpu.MemorySpace.HBM)
    vmem = pl.BlockSpec(memory_space=pltpu.VMEM)
    dma = pltpu.SemaphoreType.DMA
    updated = pl.pallas_call(
        kernel,
        out_shape=jax.ShapeDtypeStruct((64, WIDTH), BF16),
        in_specs=[hbm] * 9,
        out_specs=vmem,
        scratch_shapes=[
            pltpu.VMEM((64, WIDTH), BF16),
            pltpu.VMEM((235, 2, 128), BF16),
            pltpu.VMEM((2, 128), jnp.int32),
            pltpu.VMEM((2, 128), jnp.int32),
            pltpu.VMEM((1, 128), jnp.int32),
            pltpu.VMEM((448, 896), BF16),
            pltpu.VMEM((2, 768, 384), BF16),
            pltpu.VMEM((2, 320, 640), BF16),
            pltpu.VMEM((1, WIDTH), F32),
            pltpu.VMEM((256, 256), F32),
            pltpu.VMEM((256, ROWS), F32),
            pltpu.VMEM((WIDTH, ROWS), F32),
            pltpu.VMEM((CHUNKS, 29, 2, 64, 128), BF16),
            pltpu.VMEM((SLOTS, 2, ZERO_TILES * 128), BF16),
            pltpu.VMEM((SLOTS, 2, ZERO_TILES * 128), BF16),
            pltpu.VMEM((SLOTS, 2, REST_TILES * 128), BF16),
            pltpu.VMEM((SLOTS, 2, REST_TILES * 128), BF16),
            pltpu.VMEM((SLOTS, 2, 128), BF16),
            pltpu.VMEM((SLOTS, 2, 128), BF16),
            pltpu.VMEM((CHUNKS, 2, 128, 128), BF16),
            pltpu.VMEM((WIDTH, ROWS), BF16),
            pltpu.VMEM((64, WIDTH), F32),
            pltpu.VMEM((64, 128), F32),
            pltpu.VMEM((64, 128), F32),
            dma((9,)),
            dma((CHUNKS, 2)),
            dma((CHUNKS, 2)),
            dma((CHUNKS,)),
            dma((CHUNKS,)),
            dma((CHUNKS,)),
            dma((CHUNKS,)),
            dma((CHUNKS,)),
            dma((CHUNKS,)),
            dma((CHUNKS,)),
            dma((CHUNKS,)),
            dma((2,)),
        ],
        compiler_params=pltpu.CompilerParams(
            collective_id=0, has_side_effects=True, vmem_limit_bytes=40000000
        ),
    )(*[pltpu.with_memory_space_constraint(v, pltpu.MemorySpace.HBM) for v in (x, rt, src, dst, counts, wz, w1, w2, norm_gain)])
    return updated.reshape(64, 1, WIDTH)


def solution(mesh):
    return jax.shard_map(
        shards,
        mesh=mesh,
        in_specs=(
            P("dev", "rep", None),
            P("dev", None, None),
            P("dev", None, None),
            P("dev", None),
            P("dev", None, None, None),
            P(None, "rep", None),
            P(None, None, "rep", None),
            P(None, None, "rep", None),
            P("rep", None),
        ),
        out_specs=P("dev", "rep", None),
        check_vma=False,
    )
```

```python
import functools

import jax
import jax.numpy as jnp
from jax import lax
from jax.experimental import pallas as pl
from jax.experimental.pallas import tpu as pltpu
from jax.sharding import PartitionSpec as P

MESH = pl.DeviceIdType.MESH
F32 = jnp.float32
BF16 = jnp.bfloat16

SLOTS = 128
ROWS = 256
CHUNKS = 2
CROWS = ROWS // CHUNKS
CSLOTS = SLOTS // CHUNKS
ZERO_TILES = 4
REST_TILES = 11
TILES = ZERO_TILES + REST_TILES
WIDTH = 3136
LEAD = ((0, 1), (1, 2), (2, 3), (3, 6))
DEGREES = range(7)


def reach(l):
    return min(l, 2)


def orders(l):
    return range(-reach(l), reach(l) + 1)


def frame_slot(degree, order):
    if order == 0:
        return degree
    if order == 1:
        return 6 + degree
    if order == -1:
        return 12 + degree
    if order == 2:
        return 17 + degree
    return 22 + degree


def entry(l, a, b):
    start = sum((2 * m + 1) * (2 * reach(m) + 1) for m in range(l))
    return start + (a + reach(l)) * (2 * l + 1) + b + l


def message_places():
    place = {}
    for r in range(7):
        place[r] = (r // 2, r % 2)
    for r in range(7, 19):
        place[r] = (ZERO_TILES + (r - 7) // 2, (r - 7) % 2)
    for r in range(19, 23):
        place[r] = (ZERO_TILES + 6 + (r - 19) // 2, (r - 19) % 2)
    for r in range(24, 28):
        place[r] = (ZERO_TILES + 8 + (r - 24) // 2, (r - 24) % 2)
    place[23] = (ZERO_TILES + 10, 0)
    place[28] = (ZERO_TILES + 10, 1)
    return place


PLACE = message_places()


def nt(a, b):
    return lax.dot_general(a, b, (((1,), (1,)), ((), ())), preferred_element_type=F32)


def nn(a, b):
    return jnp.dot(a, b, preferred_element_type=F32)


def unit(n):
    rows = lax.broadcasted_iota(jnp.int32, (n, n), 0)
    cols = lax.broadcasted_iota(jnp.int32, (n, n), 1)
    return jnp.where(rows == cols, 1.0, 0.0).astype(BF16)


def kernel(
    x_hbm, rt_hbm, src_hbm, dst_hbm, cnt_hbm, wz_hbm, w1_hbm, w2_hbm, gain_hbm,
    out_ref,
    xv, rtv, srcv, dstv, cntv, wz, w1, w2, gain,
    rts, dtab, xs, rot, zsend, zrecv, msend, mrecv, dsend, drecv, dswap, sswap, back, agg, sqs, sqr,
    load_sem, ps_sem, pr_sem, zs_sem, zr_sem, ms_sem, mr_sem, ds_sem, dr_sem, ws_sem, wr_sem, vs_sem, vr_sem, q_sem,
):
    me = lax.axis_index("dev")
    rep = lax.axis_index("rep")
    px, pz, py = me // 32, (me // 4) % 8, me % 4
    barrier = pltpu.get_barrier_semaphore()

    def greet(g, carry):
        tx = (px + 2 + (g >> 2)) & 3
        ty = (py + 2 + g) & 3
        for step in (4, 3, 5, 2, 6, 1, 7):
            spot = tx * 32 + ((pz + step) & 7) * 4 + ty
            pl.semaphore_signal(barrier, inc=1, device_id={"dev": spot}, device_id_type=MESH)

        @pl.when(g != 10)
        def _():
            spot = tx * 32 + pz * 4 + ty
            pl.semaphore_signal(barrier, inc=1, device_id={"dev": spot}, device_id_type=MESH)

        return carry

    lax.fori_loop(0, 16, greet, 0)
    pl.semaphore_signal(barrier, inc=1, device_id={"rep": 1 - rep}, device_id_type=MESH)

    loads = [
        pltpu.make_async_copy(s, d, load_sem.at[i])
        for i, (s, d) in enumerate(
            [
                (rt_hbm, rtv), (src_hbm, srcv), (dst_hbm, dstv), (cnt_hbm, cntv), (x_hbm, xv),
                (wz_hbm, wz), (w1_hbm, w1), (w2_hbm, w2), (gain_hbm, gain),
            ]
        )
    ]
    for copy in loads:
        copy.start()

    def spot_of(sign):
        q = lax.broadcasted_iota(jnp.int32, (ROWS, 128), 0)
        col = lax.broadcasted_iota(jnp.int32, (ROWS, 128), 1)
        slot, i = q >> 1, q & 1
        oz, r = slot & 7, slot >> 3
        ox = r >> 2
        oy = r + ox
        tx = (px + sign * ox + 8) & 3
        tz = (pz + sign * oz + 16) & 7
        ty = (py + sign * oy + 32) & 3
        target = tx * 32 + tz * 4 + ty
        hit = jnp.where(col == target, 1, 0)
        return jnp.concatenate(
            [jnp.where(i == side, hit, 0).astype(F32).astype(BF16) for side in range(2)], axis=1
        )

    perm = spot_of(1)
    eye = unit(128)
    node = lax.broadcasted_iota(jnp.int32, (64, 128), 0)

    for copy in loads[:5]:
        copy.wait()
    hot = jnp.concatenate(
        [
            jnp.where((srcv[i : i + 1, :] == node) & (cntv[0:1, :] > i), 1.0, 0.0).astype(BF16)
            for i in range(2)
        ],
        axis=1,
    )
    hot_q = nt(hot, perm).astype(BF16)
    for t in range(25):
        wide = 128 if t < 24 else 64
        turned = nt(eye[0:wide, 0:wide], xv[:, t * 128 : t * 128 + wide]).astype(BF16)
        xs[t * 128 : t * 128 + wide, :] = nn(turned, hot_q)

    rts[...] = jnp.zeros_like(rts)
    for i in range(2):
        rts[0:235, i * 128 : (i + 1) * 128] = rtv[:, i, :].astype(F32)
    table = rts[...].astype(BF16)
    dtab[...] = nt(table, perm)
    share = rts[pl.ds(pl.multiple_of(rep * 64, 64), 64), :].astype(BF16)
    spare = nt(perm, share)
    dsend[...] = nt(perm, table[128:256]).astype(BF16).reshape(SLOTS, 2, 128)

    def lanes(c):
        return slice(c * 128, (c + 1) * 128)

    def turn(c, chosen):
        at = lanes(c)
        for l in DEGREES:
            wanted = [a for a in orders(l) if a in chosen]
            sums = {}
            for b in range(-l, l + 1):
                if wanted:
                    k = l * l + l + b
                    part = xs[k * 64 : (k + 1) * 64, at]
                for a in wanted:
                    e = entry(l, a, b)
                    term = dtab[e : e + 1, at] * part
                    sums[a] = sums[a] + term if a in sums else term
            for a in wanted:
                rot[c, frame_slot(l, a), rep] = sums[a].astype(BF16)

    def to_peer(c, part):
        rows = pl.ds(0, 7) if part == 0 else pl.ds(7, 22)
        return pltpu.make_async_remote_copy(
            src_ref=rot.at[c, rows, rep],
            dst_ref=rot.at[c, rows, rep],
            send_sem=ps_sem.at[c, part],
            recv_sem=pr_sem.at[c, part],
            device_id={"rep": 1 - rep},
            device_id_type=MESH,
        )

    def swap_table(c):
        return pltpu.make_async_remote_copy(
            src_ref=dswap.at[c],
            dst_ref=dswap.at[c],
            send_sem=ws_sem.at[c],
            recv_sem=wr_sem.at[c],
            device_id={"rep": 1 - rep},
            device_id_type=MESH,
        )

    def swap_spare(c):
        return pltpu.make_async_remote_copy(
            src_ref=sswap.at[c, rep],
            dst_ref=sswap.at[c, rep],
            send_sem=vs_sem.at[c],
            recv_sem=vr_sem.at[c],
            device_id={"rep": 1 - rep},
            device_id_type=MESH,
        )

    def send(u, plane, allowed, ordered, source, target, send_sem, recv_sem):
        r = u
        if ordered:
            row = ((u & 7) >> 1) ^ ((u & 7) >> 2)
            ox = (u >> 3) * 2 + (u & 1)
            ahead = ox * 4 + ((row - py - ox) & 3)
            r = jnp.where(plane < 4, ahead, u)
        tx = (px + (r >> 2)) & 3
        ty = (py + r + (r >> 2)) & 3
        slot = r * 8 + ((plane - pz) & 7)
        copy = pltpu.make_async_remote_copy(
            src_ref=source.at[slot],
            dst_ref=target.at[slot],
            send_sem=send_sem.at[r >> 3],
            recv_sem=recv_sem.at[r >> 3],
            device_id={"dev": tx * 32 + plane * 4 + ty},
            device_id_type=MESH,
        )

        @pl.when(allowed & (slot > 0))
        def _():
            copy.start()

    planes = [(pz + step) & 7 for step in (4, 3, 5, 2, 6, 1, 7, 0)]

    def send_steps(first, last, buffers, lead):
        def step(t, carry):
            for plane in planes:
                r = t
                for early, gap in lead:
                    r = r + jnp.where(plane == early, t // gap, 0)
                send(r, plane, r < 16, bool(lead), *buffers)
            for early, gap in lead:
                r = t + t // gap + 1
                send(r, early, (t % gap == gap - 1) & (r < 16), True, *buffers)
            return carry

        lax.fori_loop(first, last, step, 0)

    def wait_chunk(c, buffer, sem):
        part = buffer.at[pl.ds(c * CSLOTS, CSLOTS - 1 if c == 0 else CSLOTS)]
        pltpu.make_async_copy(part, part, sem.at[c]).wait()

    def rows_of(c, first, count):
        part = rot[c, first : first + count].reshape(count * 128, 128)
        return nt(eye, part).astype(BF16)

    def mix_zero():
        for c in range(CHUNKS):
            to_peer(c, 0).wait_recv()
        zero = nt(jnp.concatenate([rows_of(c, 0, 7) for c in range(CHUNKS)], axis=0), wz[...])
        message = jnp.concatenate([zero, spare], axis=1)
        zsend[...] = message.astype(BF16).reshape(SLOTS, 2, ZERO_TILES * 128)

    def mix(c):
        to_peer(c, 1).wait_recv()
        one = jnp.concatenate([rows_of(c, 7, 6), rows_of(c, 13, 6)], axis=0)
        two = jnp.concatenate([rows_of(c, 19, 5), rows_of(c, 24, 5)], axis=0)
        first, second = nn(one, w1[0]), nn(one, w1[1])
        plus1 = first[0:128] - second[128:256]
        minus1 = second[0:128] + first[128:256]
        first, second = nt(two, w2[0]), nt(two, w2[1])
        plus2 = first[0:128] - second[128:256]
        minus2 = second[0:128] + first[128:256]
        last = jnp.concatenate([plus2[:, 256:320], minus2[:, 256:320]], axis=1)
        spot = 0
        for piece in (plus1, minus1, plus2[:, 0:256], minus2[:, 0:256], last):
            wide = piece.shape[1]
            msend[c * CSLOTS : (c + 1) * CSLOTS, :, spot : spot + wide] = piece.astype(BF16).reshape(
                CSLOTS, 2, wide
            )
            spot += wide

    def table_in(c):
        @pl.when(rep == 0)
        def _():
            wait_chunk(c, drecv, dr_sem)
            if c == 0:
                drecv[0] = dsend[0]
            rows = drecv[c * CSLOTS : (c + 1) * CSLOTS].reshape(CROWS, 128)
            dswap[c] = nt(eye, rows).astype(BF16)
            swap_table(c).start()

    def tiles_in(c, buffer, count, first):
        for t in range(count):
            tile = buffer[c * CSLOTS : (c + 1) * CSLOTS, :, t * 128 : (t + 1) * 128].reshape(CROWS, 128)
            xs[(first + t) * 128 : (first + t + 1) * 128, lanes(c)] = nt(eye, tile)

    def zero_in(c):
        wait_chunk(c, zrecv, zr_sem)
        if c == 0:
            zrecv[0] = zsend[0]
        tiles_in(c, zrecv, ZERO_TILES, 0)
        sswap[c, rep] = xs[448:512, lanes(c)].astype(BF16)
        swap_spare(c).start()

    def table_done(c):
        at = lanes(c)

        @pl.when(rep == 1)
        def _():
            swap_table(c).wait_recv()

        swap_spare(c).wait_recv()
        dtab[0:64, at] = sswap[c, 0].astype(F32)
        dtab[64:128, at] = sswap[c, 1].astype(F32)
        dtab[128:256, at] = dswap[c].astype(F32)

    def unturn(c):
        at = lanes(c)
        wait_chunk(c, mrecv, mr_sem)
        if c == 0:
            mrecv[0] = msend[0]
        tiles_in(c, mrecv, REST_TILES, ZERO_TILES)
        for l in DEGREES:
            parts = {}
            for a in orders(l):
                tile, half = PLACE[frame_slot(l, a)]
                spot = (2 * tile + half) * 64
                parts[a] = xs[spot : spot + 64, at]
            for b in range(-l, l + 1):
                total = None
                for a in orders(l):
                    e = entry(l, a, b)
                    term = dtab[e : e + 1, at] * parts[a]
                    total = term if total is None else total + term
                k = l * l + l + b
                back[k * 64 : (k + 1) * 64, at] = total.astype(BF16)

    others = (-2, -1, 1, 2)
    for c in range(CHUNKS):
        turn(c, (0,))

    pl.semaphore_wait(barrier, SLOTS)
    for c in range(CHUNKS):
        to_peer(c, 0).start()

    @pl.when(rep == 0)
    def _():
        send_steps(0, 16, (dsend, drecv, ds_sem, dr_sem), ())

    for c in range(CHUNKS):
        turn(c, others)
        to_peer(c, 1).start()

    for copy in loads[5:]:
        copy.wait()
    mix_zero()
    send_steps(0, 16, (zsend, zrecv, zs_sem, zr_sem), LEAD)
    mix(0)
    send_steps(0, 4, (msend, mrecv, ms_sem, mr_sem), LEAD)
    mix(1)
    send_steps(4, 16, (msend, mrecv, ms_sem, mr_sem), LEAD)

    perm_back = spot_of(-1)
    hot_d = jnp.concatenate(
        [jnp.where(dstv[i : i + 1, :] == node, 1.0, 0.0).astype(BF16) for i in range(2)], axis=1
    )
    hot_n = nt(hot_d, perm_back).astype(BF16)

    for c in range(CHUNKS):
        table_in(c)
    for c in range(CHUNKS):
        zero_in(c)
    for c in range(CHUNKS):
        table_done(c)
    square = jnp.zeros((64, 1), F32)
    for c in range(CHUNKS):
        unturn(c)
        for s in range(7):
            at = slice(s * 448, (s + 1) * 448)
            part = nt(hot_n[:, lanes(c)], back[at, lanes(c)])
            if c > 0:
                part = agg[:, at] + part
            agg[:, at] = part
            if c == CHUNKS - 1:
                square = square + jnp.sum(part * part, axis=1, keepdims=True)
    sqs[...] = jnp.broadcast_to(square, (64, 128))
    swap = pltpu.make_async_remote_copy(
        src_ref=sqs,
        dst_ref=sqr,
        send_sem=q_sem.at[0],
        recv_sem=q_sem.at[1],
        device_id={"rep": 1 - rep},
        device_id_type=MESH,
    )
    swap.start()
    for c in range(CHUNKS):
        to_peer(c, 0).wait_send()
        to_peer(c, 1).wait_send()
        swap_spare(c).wait_send()

        @pl.when(rep == 0)
        def _():
            swap_table(c).wait_send()
            wait_chunk(c, dsend, ds_sem)

        wait_chunk(c, zsend, zs_sem)
        wait_chunk(c, msend, ms_sem)
    swap.wait()
    mean = (sqs[...] + sqr[...]) / 6272.0
    scale = lax.rsqrt(mean + 1e-06)[:, 0:1]
    for s in range(7):
        at = slice(s * 448, (s + 1) * 448)
        normed = agg[:, at] * scale
        out_ref[:, at] = (xv[:, at].astype(F32) + gain[0:1, at] * normed).astype(BF16)


def shards(node_features, src_node, dst_node, counts, rotation, w_zero, w_one, w_two, norm_gain):
    x = node_features.reshape(64, WIDTH)
    rt = rotation.transpose(0, 3, 2, 1).reshape(235, 2, 128)
    src = src_node.transpose(0, 2, 1).reshape(2, 128)
    dst = dst_node.transpose(0, 2, 1).reshape(2, 128)
    wz = w_zero.transpose(1, 2, 0).reshape(448, 896)
    w1 = w_one.reshape(2, 768, 384)
    w2 = w_two.transpose(0, 2, 3, 1).reshape(2, 320, 640)
    hbm = pl.BlockSpec(memory_space=pltpu.MemorySpace.HBM)
    vmem = pl.BlockSpec(memory_space=pltpu.VMEM)
    dma = pltpu.SemaphoreType.DMA
    updated = pl.pallas_call(
        kernel,
        out_shape=jax.ShapeDtypeStruct((64, WIDTH), BF16),
        in_specs=[hbm] * 9,
        out_specs=vmem,
        scratch_shapes=[
            pltpu.VMEM((64, WIDTH), BF16),
            pltpu.VMEM((235, 2, 128), BF16),
            pltpu.VMEM((2, 128), jnp.int32),
            pltpu.VMEM((2, 128), jnp.int32),
            pltpu.VMEM((1, 128), jnp.int32),
            pltpu.VMEM((448, 896), BF16),
            pltpu.VMEM((2, 768, 384), BF16),
            pltpu.VMEM((2, 320, 640), BF16),
            pltpu.VMEM((1, WIDTH), F32),
            pltpu.VMEM((256, 256), F32),
            pltpu.VMEM((256, ROWS), F32),
            pltpu.VMEM((WIDTH, ROWS), F32),
            pltpu.VMEM((CHUNKS, 29, 2, 64, 128), BF16),
            pltpu.VMEM((SLOTS, 2, ZERO_TILES * 128), BF16),
            pltpu.VMEM((SLOTS, 2, ZERO_TILES * 128), BF16),
            pltpu.VMEM((SLOTS, 2, REST_TILES * 128), BF16),
            pltpu.VMEM((SLOTS, 2, REST_TILES * 128), BF16),
            pltpu.VMEM((SLOTS, 2, 128), BF16),
            pltpu.VMEM((SLOTS, 2, 128), BF16),
            pltpu.VMEM((CHUNKS, 128, 128), BF16),
            pltpu.VMEM((CHUNKS, 2, 64, 128), BF16),
            pltpu.VMEM((WIDTH, ROWS), BF16),
            pltpu.VMEM((64, WIDTH), F32),
            pltpu.VMEM((64, 128), F32),
            pltpu.VMEM((64, 128), F32),
            dma((9,)),
            dma((CHUNKS, 2)),
            dma((CHUNKS, 2)),
            dma((CHUNKS,)),
            dma((CHUNKS,)),
            dma((CHUNKS,)),
            dma((CHUNKS,)),
            dma((CHUNKS,)),
            dma((CHUNKS,)),
            dma((CHUNKS,)),
            dma((CHUNKS,)),
            dma((CHUNKS,)),
            dma((CHUNKS,)),
            dma((2,)),
        ],
        compiler_params=pltpu.CompilerParams(
            collective_id=0, has_side_effects=True, vmem_limit_bytes=40000000
        ),
    )(*[pltpu.with_memory_space_constraint(v, pltpu.MemorySpace.HBM) for v in (x, rt, src, dst, counts, wz, w1, w2, norm_gain)])
    return updated.reshape(64, 1, WIDTH)


def solution(mesh):
    return jax.shard_map(
        shards,
        mesh=mesh,
        in_specs=(
            P("dev", "rep", None),
            P("dev", None, None),
            P("dev", None, None),
            P("dev", None),
            P("dev", None, None, None),
            P(None, "rep", None),
            P(None, None, "rep", None),
            P(None, None, "rep", None),
            P("rep", None),
        ),
        out_specs=P("dev", "rep", None),
        check_vma=False,
    )
```

```python
import functools

import jax
import jax.numpy as jnp
from jax import lax
from jax.experimental import pallas as pl
from jax.experimental.pallas import tpu as pltpu
from jax.sharding import PartitionSpec as P

MESH = pl.DeviceIdType.MESH
F32 = jnp.float32
BF16 = jnp.bfloat16

SLOTS = 128
ROWS = 256
CHUNKS = 2
CROWS = ROWS // CHUNKS
CSLOTS = SLOTS // CHUNKS
ZERO_TILES = 4
REST_TILES = 11
TILES = ZERO_TILES + REST_TILES
WIDTH = 3136
LEAD = ((0, 1), (1, 2), (2, 3), (3, 6))
DEGREES = range(7)


def reach(l):
    return min(l, 2)


def orders(l):
    return range(-reach(l), reach(l) + 1)


def frame_slot(degree, order):
    if order == 0:
        return degree
    if order == 1:
        return 6 + degree
    if order == -1:
        return 12 + degree
    if order == 2:
        return 17 + degree
    return 22 + degree


def entry(l, a, b):
    start = sum((2 * m + 1) * (2 * reach(m) + 1) for m in range(l))
    return start + (a + reach(l)) * (2 * l + 1) + b + l


def message_places():
    place = {}
    for r in range(7):
        place[r] = (r // 2, r % 2)
    for r in range(7, 19):
        place[r] = (ZERO_TILES + (r - 7) // 2, (r - 7) % 2)
    for r in range(19, 23):
        place[r] = (ZERO_TILES + 6 + (r - 19) // 2, (r - 19) % 2)
    for r in range(24, 28):
        place[r] = (ZERO_TILES + 8 + (r - 24) // 2, (r - 24) % 2)
    place[23] = (ZERO_TILES + 10, 0)
    place[28] = (ZERO_TILES + 10, 1)
    return place


PLACE = message_places()


def nt(a, b):
    return lax.dot_general(a, b, (((1,), (1,)), ((), ())), preferred_element_type=F32)


def nn(a, b):
    return jnp.dot(a, b, preferred_element_type=F32)


def unit(n):
    rows = lax.broadcasted_iota(jnp.int32, (n, n), 0)
    cols = lax.broadcasted_iota(jnp.int32, (n, n), 1)
    return jnp.where(rows == cols, 1.0, 0.0).astype(BF16)


def kernel(
    x_hbm, rt_hbm, src_hbm, dst_hbm, cnt_hbm, wz_hbm, w1_hbm, w2_hbm, gain_hbm,
    out_ref,
    xv, rtv, srcv, dstv, cntv, wz, w1, w2, gain,
    rts, dtab, xs, rot, zsend, zrecv, msend, mrecv, dsend, drecv, dswap, sswap, back, agg, sqs, sqr,
    load_sem, ps_sem, pr_sem, zs_sem, zr_sem, ms_sem, mr_sem, ds_sem, dr_sem, ws_sem, wr_sem, vs_sem, vr_sem, q_sem,
):
    me = lax.axis_index("dev")
    rep = lax.axis_index("rep")
    px, pz, py = me // 32, (me // 4) % 8, me % 4
    barrier = pltpu.get_barrier_semaphore()

    def greet(g, carry):
        tx = (px + 2 + (g >> 2)) & 3
        ty = (py + 2 + g) & 3
        for step in (4, 3, 5, 2, 6, 1, 7):
            spot = tx * 32 + ((pz + step) & 7) * 4 + ty
            pl.semaphore_signal(barrier, inc=1, device_id={"dev": spot}, device_id_type=MESH)

        @pl.when(g != 10)
        def _():
            spot = tx * 32 + pz * 4 + ty
            pl.semaphore_signal(barrier, inc=1, device_id={"dev": spot}, device_id_type=MESH)

        return carry

    for g in range(16):
        greet(g, 0)
    pl.semaphore_signal(barrier, inc=1, device_id={"rep": 1 - rep}, device_id_type=MESH)

    loads = [
        pltpu.make_async_copy(s, d, load_sem.at[i])
        for i, (s, d) in enumerate(
            [
                (rt_hbm, rtv), (src_hbm, srcv), (dst_hbm, dstv), (cnt_hbm, cntv), (x_hbm, xv),
                (wz_hbm, wz), (w1_hbm, w1), (w2_hbm, w2), (gain_hbm, gain),
            ]
        )
    ]
    for copy in loads:
        copy.start()

    def spot_of(sign):
        q = lax.broadcasted_iota(jnp.int32, (ROWS, 128), 0)
        col = lax.broadcasted_iota(jnp.int32, (ROWS, 128), 1)
        slot, i = q >> 1, q & 1
        oz, r = slot & 7, slot >> 3
        ox = r >> 2
        oy = r + ox
        tx = (px + sign * ox + 8) & 3
        tz = (pz + sign * oz + 16) & 7
        ty = (py + sign * oy + 32) & 3
        target = tx * 32 + tz * 4 + ty
        hit = jnp.where(col == target, 1, 0)
        return jnp.concatenate(
            [jnp.where(i == side, hit, 0).astype(F32).astype(BF16) for side in range(2)], axis=1
        )

    perm = spot_of(1)
    eye = unit(128)
    node = lax.broadcasted_iota(jnp.int32, (64, 128), 0)

    for copy in loads[:5]:
        copy.wait()
    hot = jnp.concatenate(
        [
            jnp.where((srcv[i : i + 1, :] == node) & (cntv[0:1, :] > i), 1.0, 0.0).astype(BF16)
            for i in range(2)
        ],
        axis=1,
    )
    hot_q = nt(hot, perm).astype(BF16)
    for t in range(25):
        wide = 128 if t < 24 else 64
        turned = nt(eye[0:wide, 0:wide], xv[:, t * 128 : t * 128 + wide]).astype(BF16)
        xs[t * 128 : t * 128 + wide, :] = nn(turned, hot_q)

    rts[...] = jnp.zeros_like(rts)
    for i in range(2):
        rts[0:235, i * 128 : (i + 1) * 128] = rtv[:, i, :].astype(F32)
    table = rts[...].astype(BF16)
    dtab[...] = nt(table, perm)
    share = rts[pl.ds(pl.multiple_of(rep * 64, 64), 64), :].astype(BF16)
    spare = nt(perm, share)
    dsend[...] = nt(perm, table[128:256]).astype(BF16).reshape(SLOTS, 2, 128)

    def lanes(c):
        return slice(c * 128, (c + 1) * 128)

    def turn(c, chosen):
        at = lanes(c)
        for l in DEGREES:
            wanted = [a for a in orders(l) if a in chosen]
            sums = {}
            for b in range(-l, l + 1):
                if wanted:
                    k = l * l + l + b
                    part = xs[k * 64 : (k + 1) * 64, at]
                for a in wanted:
                    e = entry(l, a, b)
                    term = dtab[e : e + 1, at] * part
                    sums[a] = sums[a] + term if a in sums else term
            for a in wanted:
                rot[c, frame_slot(l, a), rep] = sums[a].astype(BF16)

    def to_peer(c, part):
        rows = pl.ds(0, 7) if part == 0 else pl.ds(7, 22)
        return pltpu.make_async_remote_copy(
            src_ref=rot.at[c, rows, rep],
            dst_ref=rot.at[c, rows, rep],
            send_sem=ps_sem.at[c, part],
            recv_sem=pr_sem.at[c, part],
            device_id={"rep": 1 - rep},
            device_id_type=MESH,
        )

    def swap_table(c):
        return pltpu.make_async_remote_copy(
            src_ref=dswap.at[c],
            dst_ref=dswap.at[c],
            send_sem=ws_sem.at[c],
            recv_sem=wr_sem.at[c],
            device_id={"rep": 1 - rep},
            device_id_type=MESH,
        )

    def swap_spare(c):
        return pltpu.make_async_remote_copy(
            src_ref=sswap.at[c, rep],
            dst_ref=sswap.at[c, rep],
            send_sem=vs_sem.at[c],
            recv_sem=vr_sem.at[c],
            device_id={"rep": 1 - rep},
            device_id_type=MESH,
        )

    def send(u, plane, allowed, ordered, source, target, send_sem, recv_sem):
        r = u
        if ordered:
            row = ((u & 7) >> 1) ^ ((u & 7) >> 2)
            ox = (u >> 3) * 2 + (u & 1)
            ahead = ox * 4 + ((row - py - ox) & 3)
            r = jnp.where(plane < 4, ahead, u)
        tx = (px + (r >> 2)) & 3
        ty = (py + r + (r >> 2)) & 3
        slot = r * 8 + ((plane - pz) & 7)
        copy = pltpu.make_async_remote_copy(
            src_ref=source.at[slot],
            dst_ref=target.at[slot],
            send_sem=send_sem.at[r >> 3],
            recv_sem=recv_sem.at[r >> 3],
            device_id={"dev": tx * 32 + plane * 4 + ty},
            device_id_type=MESH,
        )

        @pl.when(allowed & (slot > 0))
        def _():
            copy.start()

    planes = [(pz + step) & 7 for step in (4, 3, 5, 2, 6, 1, 7, 0)]

    def send_steps(first, last, buffers, lead):
        def step(t, carry):
            for plane in planes:
                r = t
                for early, gap in lead:
                    r = r + jnp.where(plane == early, t // gap, 0)
                send(r, plane, r < 16, bool(lead), *buffers)
            for early, gap in lead:
                r = t + t // gap + 1
                send(r, early, (t % gap == gap - 1) & (r < 16), True, *buffers)
            return carry

        lax.fori_loop(first, last, step, 0)

    def wait_chunk(c, buffer, sem):
        part = buffer.at[pl.ds(c * CSLOTS, CSLOTS - 1 if c == 0 else CSLOTS)]
        pltpu.make_async_copy(part, part, sem.at[c]).wait()

    def rows_of(c, first, count):
        part = rot[c, first : first + count].reshape(count * 128, 128)
        return nt(eye, part).astype(BF16)

    def mix_zero():
        for c in range(CHUNKS):
            to_peer(c, 0).wait_recv()
        zero = nt(jnp.concatenate([rows_of(c, 0, 7) for c in range(CHUNKS)], axis=0), wz[...])
        message = jnp.concatenate([zero, spare], axis=1)
        zsend[...] = message.astype(BF16).reshape(SLOTS, 2, ZERO_TILES * 128)

    def mix(c):
        to_peer(c, 1).wait_recv()
        one = jnp.concatenate([rows_of(c, 7, 6), rows_of(c, 13, 6)], axis=0)
        two = jnp.concatenate([rows_of(c, 19, 5), rows_of(c, 24, 5)], axis=0)
        first, second = nn(one, w1[0]), nn(one, w1[1])
        plus1 = first[0:128] - second[128:256]
        minus1 = second[0:128] + first[128:256]
        first, second = nt(two, w2[0]), nt(two, w2[1])
        plus2 = first[0:128] - second[128:256]
        minus2 = second[0:128] + first[128:256]
        last = jnp.concatenate([plus2[:, 256:320], minus2[:, 256:320]], axis=1)
        spot = 0
        for piece in (plus1, minus1, plus2[:, 0:256], minus2[:, 0:256], last):
            wide = piece.shape[1]
            msend[c * CSLOTS : (c + 1) * CSLOTS, :, spot : spot + wide] = piece.astype(BF16).reshape(
                CSLOTS, 2, wide
            )
            spot += wide

    def table_in(c):
        @pl.when(rep == 0)
        def _():
            wait_chunk(c, drecv, dr_sem)
            if c == 0:
                drecv[0] = dsend[0]
            rows = drecv[c * CSLOTS : (c + 1) * CSLOTS].reshape(CROWS, 128)
            dswap[c] = nt(eye, rows).astype(BF16)
            swap_table(c).start()

    def tiles_in(c, buffer, count, first):
        for t in range(count):
            tile = buffer[c * CSLOTS : (c + 1) * CSLOTS, :, t * 128 : (t + 1) * 128].reshape(CROWS, 128)
            xs[(first + t) * 128 : (first + t + 1) * 128, lanes(c)] = nt(eye, tile)

    def zero_in(c):
        wait_chunk(c, zrecv, zr_sem)
        if c == 0:
            zrecv[0] = zsend[0]
        tiles_in(c, zrecv, ZERO_TILES, 0)
        sswap[c, rep] = xs[448:512, lanes(c)].astype(BF16)
        swap_spare(c).start()

    def table_done(c):
        at = lanes(c)

        @pl.when(rep == 1)
        def _():
            swap_table(c).wait_recv()

        swap_spare(c).wait_recv()
        dtab[0:64, at] = sswap[c, 0].astype(F32)
        dtab[64:128, at] = sswap[c, 1].astype(F32)
        dtab[128:256, at] = dswap[c].astype(F32)

    def unturn(c):
        at = lanes(c)
        wait_chunk(c, mrecv, mr_sem)
        if c == 0:
            mrecv[0] = msend[0]
        tiles_in(c, mrecv, REST_TILES, ZERO_TILES)
        for l in DEGREES:
            parts = {}
            for a in orders(l):
                tile, half = PLACE[frame_slot(l, a)]
                spot = (2 * tile + half) * 64
                parts[a] = xs[spot : spot + 64, at]
            for b in range(-l, l + 1):
                total = None
                for a in orders(l):
                    e = entry(l, a, b)
                    term = dtab[e : e + 1, at] * parts[a]
                    total = term if total is None else total + term
                k = l * l + l + b
                back[k * 64 : (k + 1) * 64, at] = total.astype(BF16)

    others = (-2, -1, 1, 2)
    for c in range(CHUNKS):
        turn(c, (0,))

    pl.semaphore_wait(barrier, SLOTS)
    for c in range(CHUNKS):
        to_peer(c, 0).start()

    @pl.when(rep == 0)
    def _():
        send_steps(0, 16, (dsend, drecv, ds_sem, dr_sem), ())

    for c in range(CHUNKS):
        turn(c, others)
        to_peer(c, 1).start()

    for copy in loads[5:]:
        copy.wait()
    mix_zero()
    send_steps(0, 16, (zsend, zrecv, zs_sem, zr_sem), LEAD)
    mix(0)
    send_steps(0, 4, (msend, mrecv, ms_sem, mr_sem), LEAD)
    mix(1)
    send_steps(4, 16, (msend, mrecv, ms_sem, mr_sem), LEAD)

    perm_back = spot_of(-1)
    hot_d = jnp.concatenate(
        [jnp.where(dstv[i : i + 1, :] == node, 1.0, 0.0).astype(BF16) for i in range(2)], axis=1
    )
    hot_n = nt(hot_d, perm_back).astype(BF16)

    for c in range(CHUNKS):
        table_in(c)
    for c in range(CHUNKS):
        zero_in(c)
    for c in range(CHUNKS):
        table_done(c)
    square = jnp.zeros((64, 1), F32)
    for c in range(CHUNKS):
        unturn(c)
        for s in range(7):
            at = slice(s * 448, (s + 1) * 448)
            part = nt(hot_n[:, lanes(c)], back[at, lanes(c)])
            if c > 0:
                part = agg[:, at] + part
            agg[:, at] = part
            if c == CHUNKS - 1:
                square = square + jnp.sum(part * part, axis=1, keepdims=True)
    sqs[...] = jnp.broadcast_to(square, (64, 128))
    swap = pltpu.make_async_remote_copy(
        src_ref=sqs,
        dst_ref=sqr,
        send_sem=q_sem.at[0],
        recv_sem=q_sem.at[1],
        device_id={"rep": 1 - rep},
        device_id_type=MESH,
    )
    swap.start()
    for c in range(CHUNKS):
        to_peer(c, 0).wait_send()
        to_peer(c, 1).wait_send()
        swap_spare(c).wait_send()

        @pl.when(rep == 0)
        def _():
            swap_table(c).wait_send()
            wait_chunk(c, dsend, ds_sem)

        wait_chunk(c, zsend, zs_sem)
        wait_chunk(c, msend, ms_sem)
    swap.wait()
    mean = (sqs[...] + sqr[...]) / 6272.0
    scale = lax.rsqrt(mean + 1e-06)[:, 0:1]
    for s in range(7):
        at = slice(s * 448, (s + 1) * 448)
        normed = agg[:, at] * scale
        out_ref[:, at] = (xv[:, at].astype(F32) + gain[0:1, at] * normed).astype(BF16)


def shards(node_features, src_node, dst_node, counts, rotation, w_zero, w_one, w_two, norm_gain):
    x = node_features.reshape(64, WIDTH)
    rt = rotation.transpose(0, 3, 2, 1).reshape(235, 2, 128)
    src = src_node.transpose(0, 2, 1).reshape(2, 128)
    dst = dst_node.transpose(0, 2, 1).reshape(2, 128)
    wz = w_zero.transpose(1, 2, 0).reshape(448, 896)
    w1 = w_one.reshape(2, 768, 384)
    w2 = w_two.transpose(0, 2, 3, 1).reshape(2, 320, 640)
    hbm = pl.BlockSpec(memory_space=pltpu.MemorySpace.HBM)
    vmem = pl.BlockSpec(memory_space=pltpu.VMEM)
    dma = pltpu.SemaphoreType.DMA
    updated = pl.pallas_call(
        kernel,
        out_shape=jax.ShapeDtypeStruct((64, WIDTH), BF16),
        in_specs=[hbm] * 9,
        out_specs=vmem,
        scratch_shapes=[
            pltpu.VMEM((64, WIDTH), BF16),
            pltpu.VMEM((235, 2, 128), BF16),
            pltpu.VMEM((2, 128), jnp.int32),
            pltpu.VMEM((2, 128), jnp.int32),
            pltpu.VMEM((1, 128), jnp.int32),
            pltpu.VMEM((448, 896), BF16),
            pltpu.VMEM((2, 768, 384), BF16),
            pltpu.VMEM((2, 320, 640), BF16),
            pltpu.VMEM((1, WIDTH), F32),
            pltpu.VMEM((256, 256), F32),
            pltpu.VMEM((256, ROWS), F32),
            pltpu.VMEM((WIDTH, ROWS), F32),
            pltpu.VMEM((CHUNKS, 29, 2, 64, 128), BF16),
            pltpu.VMEM((SLOTS, 2, ZERO_TILES * 128), BF16),
            pltpu.VMEM((SLOTS, 2, ZERO_TILES * 128), BF16),
            pltpu.VMEM((SLOTS, 2, REST_TILES * 128), BF16),
            pltpu.VMEM((SLOTS, 2, REST_TILES * 128), BF16),
            pltpu.VMEM((SLOTS, 2, 128), BF16),
            pltpu.VMEM((SLOTS, 2, 128), BF16),
            pltpu.VMEM((CHUNKS, 128, 128), BF16),
            pltpu.VMEM((CHUNKS, 2, 64, 128), BF16),
            pltpu.VMEM((WIDTH, ROWS), BF16),
            pltpu.VMEM((64, WIDTH), F32),
            pltpu.VMEM((64, 128), F32),
            pltpu.VMEM((64, 128), F32),
            dma((9,)),
            dma((CHUNKS, 2)),
            dma((CHUNKS, 2)),
            dma((CHUNKS,)),
            dma((CHUNKS,)),
            dma((CHUNKS,)),
            dma((CHUNKS,)),
            dma((CHUNKS,)),
            dma((CHUNKS,)),
            dma((CHUNKS,)),
            dma((CHUNKS,)),
            dma((CHUNKS,)),
            dma((CHUNKS,)),
            dma((2,)),
        ],
        compiler_params=pltpu.CompilerParams(
            collective_id=0, has_side_effects=True, vmem_limit_bytes=40000000
        ),
    )(*[pltpu.with_memory_space_constraint(v, pltpu.MemorySpace.HBM) for v in (x, rt, src, dst, counts, wz, w1, w2, norm_gain)])
    return updated.reshape(64, 1, WIDTH)


def solution(mesh):
    return jax.shard_map(
        shards,
        mesh=mesh,
        in_specs=(
            P("dev", "rep", None),
            P("dev", None, None),
            P("dev", None, None),
            P("dev", None),
            P("dev", None, None, None),
            P(None, "rep", None),
            P(None, None, "rep", None),
            P(None, None, "rep", None),
            P("rep", None),
        ),
        out_specs=P("dev", "rep", None),
        check_vma=False,
    )
```
